32 devices in a mesh: mol: 2 (over x), pts: 16 (over z, y, core).
Axes of the slice: x: 2, y: 2, z: 4, core: 2. Of those that a mesh axis runs over, the one named last changes fastest.
Arguments:
- points_map: bfloat16 [12800, 800], P(('mol', 'pts')), parts along dimension 0, may hold values from -0.21875 to 0.21875
- trial: bfloat16 [12800, 128], P('mol'), parts along dimension 0, may hold values from -6 to 6
- core: bfloat16 [12800, 6400], P(('mol', 'pts')), parts along dimension 0, may hold values from -2 to 4, as said below
- walkers: bfloat16 [1600, 12, 128], P('mol'), parts along dimension 0, may hold values from -6 to 6
- draws: int32 [12800, 12], P(('mol', 'pts')), parts along dimension 0, may hold values from 0 to 3
Outputs:
- new_walkers: bfloat16 [1600, 12, 128], P(('mol', 'pts')), parts along dimension 0
- energy: float32 [24], P('mol'), parts along dimension 0
The draws below stay inside these ranges and needn't reach their ends.
There are 2 independent parts, one for each index of `mol`. The reference program is written for one: setup_inputs(seed, part) draws one part's arguments, and reference() takes and returns one part's arrays. A program takes and returns all parts, laid end to end along the dimension named above; each array names one. Nothing has to cross between parts.
Inputs may be any that keep to these rules, and one draw needn't show every extreme that they name: core is symmetric.
All inputs are finite; a program needn't handle non-finite values.
Results may differ from the reference program's by a relative error of at most 0.018.
Values may be sent and summed in bfloat16 or wider, within the bound.
A program may use at most 192 MiB of HBM per device.

```python
import math
import jax
import jax.numpy as jnp
from jax import lax

N = 800
NOCC = 128
POINTS = 6400
WALKERS = 12
TAYLOR = 3


def draw_core(key, part):
    first_key = jax.random.fold_in(jax.random.fold_in(key, 11), 0)
    gauss = jax.random.normal(first_key, (POINTS, POINTS), jnp.float32)
    matrix = (gauss + gauss.T) / math.sqrt(2.0 * POINTS)
    matrix = matrix + jnp.eye(POINTS, dtype=jnp.float32)
    return matrix.astype(jnp.bfloat16)


def with_ends(drawn, key, smallest, largest):
    longest = drawn.shape.index(max(drawn.shape))
    spots = []
    for shift in (0, 1):
        where = [jax.random.randint(jax.random.fold_in(key, axis), (), 0, length) for axis, length in enumerate(drawn.shape)]
        where[longest] = (where[longest] + shift) % drawn.shape[longest]
        spots.append(tuple(where))
    return drawn.at[spots[0]].set(smallest).at[spots[1]].set(largest)


def shard_levels(stream_key, extent, pieces, least, high):
    gain, own = 1.0, jax.random.fold_in(stream_key, 6)
    for position, blocks in pieces:
        steps = jnp.exp(jax.random.uniform(jax.random.fold_in(own, position), (blocks,), jnp.float32, least / len(pieces), high / len(pieces)))
        gain = gain * jnp.repeat(steps, extent[position] // blocks).reshape([-1 if axis == position else 1 for axis in range(len(extent))])
    return gain


def scatter_about(own_key, extent, scale, bound, cuts=(), kind=jnp.bfloat16):
    loudness = shard_levels(own_key, extent, cuts, -0.22, 0.18) if cuts else 1.0
    values = jax.random.normal(own_key, extent, jnp.float32) * scale * loudness
    return jnp.minimum(jnp.maximum(values, -bound), bound).astype(kind)


def setup_inputs(seed: int = 0, part: int = 0) -> dict:
    key_list = jax.random.split(jax.random.key(seed), 6)
    own_keys = jax.random.split(jax.random.fold_in(key_list[5], part), 6)
    points_map = scatter_about(own_keys[0], (POINTS, N), N ** -0.5, 0.21875, ((0, 16),))
    trial = scatter_about(own_keys[1], (POINTS, NOCC), 1.0, 6.0)
    core = draw_core(jax.random.fold_in(jax.random.fold_in(key_list[5], part), 71), part)
    walkers = scatter_about(own_keys[3], (N, WALKERS, NOCC), 1.0, 6.0)
    draws = with_ends(jax.random.randint(own_keys[4], (POINTS, WALKERS), 0, 4), jax.random.fold_in(own_keys[4], 1), 0, 3).astype(jnp.int32)
    return dict(points_map=points_map, trial=trial, core=core, walkers=walkers, draws=draws)


GAUSS_NODES = (-2.3344142, -0.7419637, 0.7419637, 2.3344142)
FIELD_STEP = 0.15

def node_lookup(draws):
    values = jnp.zeros(draws.shape, jnp.float32)
    for number, node in enumerate(GAUSS_NODES):
        values = values + jnp.where(draws == number, node, 0.0).astype(jnp.float32)
    return values

def reference(points_map, trial, core, walkers, draws):
    flat_walkers = walkers.reshape(N, WALKERS * NOCC)
    orbit = jnp.dot(points_map, flat_walkers, preferred_element_type=jnp.float32).astype(jnp.bfloat16).reshape(POINTS, WALKERS, NOCC)
    density = (lax.optimization_barrier(jnp.sum(orbit.astype(jnp.float32) * trial.astype(jnp.float32)[:, None, :], axis=2)) / math.sqrt(NOCC)).astype(jnp.bfloat16)
    potential = jnp.dot(core, density, preferred_element_type=jnp.float32)
    field = FIELD_STEP * (node_lookup(draws) - FIELD_STEP * potential)
    running = walkers.astype(jnp.float32)
    current = orbit
    term_now = walkers
    for degree in range(1, TAYLOR + 1):
        if degree > 1:
            current = jnp.dot(points_map, term_now.reshape(N, WALKERS * NOCC), preferred_element_type=jnp.float32).astype(jnp.bfloat16).reshape(POINTS, WALKERS, NOCC)
        scaled = (field[:, :, None] * current.astype(jnp.float32)).astype(jnp.bfloat16).reshape(POINTS, WALKERS * NOCC)
        summed = jnp.einsum('pi,pc->ic', points_map.astype(jnp.float32), scaled.astype(jnp.float32))
        term_now = (summed / degree).astype(jnp.bfloat16).reshape(N, WALKERS, NOCC)
        running = running + term_now.astype(jnp.float32)
    new_walkers = running.astype(jnp.bfloat16)
    hartree = lax.optimization_barrier(jnp.sum(density.astype(jnp.float32) * potential, axis=0))
    core_wide = core.astype(jnp.float32)

    def per_walker(orbit_walker):
        mixed = jnp.dot(orbit_walker, trial.T, preferred_element_type=jnp.float32)
        return jnp.sum(core_wide * mixed * mixed.T) / NOCC
    exchange = lax.map(per_walker, jnp.moveaxis(orbit, 1, 0))
    energy = (hartree - exchange) / (2.0 * POINTS)
    return (new_walkers, energy)
```

```python
import functools
import math

import jax
import jax.numpy as jnp
from jax import lax
from jax.experimental import pallas as pl
from jax.experimental.pallas import tpu as pltpu
from jax.sharding import PartitionSpec as P

TAYLOR = 3


GAUSS_NODES = (-2.3344142, -0.7419637, 0.7419637, 2.3344142)
FIELD_STEP = 0.15
LANES = 128
CONTRACT_LAST = (((1,), (1,)), ((), ()))
CONTRACT_FIRST = (((0,), (0,)), ((), ()))


def node_lookup(draws):
    values = jnp.zeros(draws.shape, jnp.float32)
    for number, node in enumerate(GAUSS_NODES):
        values = values + jnp.where(draws == number, node, 0.0).astype(jnp.float32)
    return values


def dot(left, right, dims):
    return lax.dot_general(left, right, dims, preferred_element_type=jnp.float32)


def fused_kernel(
    n, walker_count, map_hbm, trial_hbm, core_hbm, walkers_hbm, draws_ref, out_ref, energy_ref,
    gathered, trial_ref, core_ref, walkers_ref, orbit_own, blocks, sums, total, term,
    dens_own, dens_slots, dens_full, field_own, field_slots, fields, chosen, energy_own, energy_slots, pick, outgoing, incoming,
    local_sems, right_sems, left_sems, side_sems, recv_sems, dens_sems, field_sems, energy_sems, out_sems,
):
    rows, columns = orbit_own.shape
    occupied = trial_ref.shape[1]
    own, orbitals = total.shape
    points = gathered.shape[0]
    window = blocks.shape[0]
    own_rows = out_ref.shape[0]
    lines = dens_own.shape[0]
    span = chosen.shape[0]
    chips = n // 2
    far = chips // 2
    top = (rows // 2 + 15) // 16 * 16
    parts = ((0, top), (top, rows - top))
    me = lax.axis_index("pts")
    core_id = lax.rem(me, 2)
    chip = me // 2
    ring = jnp.where(lax.rem(chip, 2) == 0, chip // 2, chips - 1 - chip // 2)

    def device(place, side):
        place = lax.rem(place + 2 * chips, chips)
        where = jnp.where(place < far, 2 * place, 2 * (chips - 1 - place) + 1)
        return 2 * where + side

    right, left, partner = device(ring + 1, core_id), device(ring - 1, core_id), device(ring, 1 - core_id)

    def rows_of(index):
        return pl.ds(pl.multiple_of(index * rows, 16), rows)

    def slot(index, part=None):
        offset, length = (0, rows) if part is None else parts[part]
        return gathered.at[pl.ds(pl.multiple_of(index * rows + offset, 16), length), :]

    def remote(src, dst, send_sem, recv_sem, target):
        return pltpu.make_async_remote_copy(
            src_ref=src,
            dst_ref=dst,
            send_sem=send_sem,
            recv_sem=recv_sem,
            device_id={"pts": target},
            device_id_type=pl.DeviceIdType.MESH,
        )

    def send(index, part, send_sem, target):
        return remote(slot(index, part), slot(index, part), send_sem, recv_sems.at[index, part or 0], target)

    def forward(index, part, send_sem, target):
        send(index, part, send_sem, target).start()

    def arrived(index, part=None):
        send(index, part, side_sems.at[0, 0], partner).wait_recv()

    def to_everyone(source, slots, sems):
        for step in range(1, n):
            peer = lax.rem(me + step, n)
            remote(source(peer), slots.at[me], sems.at[0, step], sems.at[1, me], peer).start()

    def from_everyone(source, slots, sems):
        for step in range(1, n):
            peer = lax.rem(me + step, n)
            remote(source(peer), slots.at[peer], sems.at[0, step], sems.at[1, peer], peer).wait_recv()

    def all_sent(source, slots, sems):
        for step in range(1, n):
            peer = lax.rem(me + step, n)
            remote(source(peer), slots.at[me], sems.at[0, step], sems.at[1, me], peer).wait_send()

    own_here = rows_of(me)
    local = [
        pltpu.make_async_copy(map_hbm, gathered.at[own_here, :], local_sems.at[0]),
        pltpu.make_async_copy(walkers_hbm, walkers_ref, local_sems.at[1]),
        pltpu.make_async_copy(trial_hbm, trial_ref, local_sems.at[2]),
        pltpu.make_async_copy(core_hbm, core_ref, local_sems.at[3]),
    ]
    for copy in local:
        copy.start()
    barrier = pltpu.get_barrier_semaphore()
    for step in range(1, n):
        pl.semaphore_signal(
            barrier, inc=1, device_id={"pts": lax.rem(me + step, n)}, device_id_type=pl.DeviceIdType.MESH
        )
    sums[...] = jnp.zeros_like(sums)
    total[...] = jnp.zeros_like(total)
    local[0].wait()
    pl.semaphore_wait(barrier, n - 1)
    send(me, None, right_sems.at[0], right).start()
    send(me, None, left_sems.at[0], left).start()
    send(me, None, side_sems.at[0, 0], partner).start()

    local[1].wait()
    local[2].wait()
    orbit_own[...] = dot(gathered[own_here, :], walkers_ref[...], (((1,), (0,)), ((), ()))).astype(jnp.bfloat16)
    trial_own = trial_ref[own_here, :].astype(jnp.float32)
    lane = lax.broadcasted_iota(jnp.int32, (rows, LANES), 1)
    density = jnp.zeros((rows, LANES), jnp.float32)
    for walker in range(walker_count):
        cols = slice(walker * occupied, (walker + 1) * occupied)
        column = jnp.sum(orbit_own[:, cols].astype(jnp.float32) * trial_own, axis=1, keepdims=True)
        density = jnp.where(lane == walker, column, density)
    density = (density / math.sqrt(occupied)).astype(jnp.bfloat16)
    unit = (
        lax.broadcasted_iota(jnp.int32, (lines, LANES), 0) == lax.broadcasted_iota(jnp.int32, (lines, LANES), 1)
    ).astype(jnp.bfloat16)
    density_t = dot(unit, density, CONTRACT_LAST)

    def placed(index):
        return pl.multiple_of(index * rows // LANES * LANES, LANES), lax.rem(index * rows, LANES)

    base, shift = placed(me)
    field_own[...] = jnp.zeros_like(field_own)
    field_own[:, :rows] = density_t
    shifted = pltpu.roll(field_own[...], shift, 1).astype(jnp.bfloat16)
    dens_own[...] = shifted
    dens_slots[me] = shifted
    to_everyone(lambda peer: dens_own, dens_slots, dens_sems)

    start = me * own
    left_col = pl.multiple_of(jnp.minimum(start // LANES * LANES, columns - 2 * LANES), LANES)
    choose = (
        lax.broadcasted_iota(jnp.int32, (own, 2 * LANES), 0) + (start - left_col)
        == lax.broadcasted_iota(jnp.int32, (own, 2 * LANES), 1)
    ).astype(jnp.bfloat16)
    cols_own = dot(choose, walkers_ref[:, pl.ds(left_col, 2 * LANES)], CONTRACT_LAST).astype(jnp.bfloat16)
    term[...] = cols_own
    running = cols_own.astype(jnp.float32)
    out_line = lax.broadcasted_iota(jnp.int32, pick.shape, 0)
    out_row = lax.rem(out_line, outgoing.shape[1])
    wanted = jnp.where(out_row < own_rows, out_line // outgoing.shape[1] * own_rows + out_row, -1)
    pick[...] = (wanted == lax.broadcasted_iota(jnp.int32, pick.shape, 1)).astype(jnp.bfloat16)
    local[3].wait()

    def exchange(pair, weight):
        first = pair * rows
        block_base, block_shift = placed(pair)
        block_shift = pl.multiple_of(block_shift, 16)
        blocks[...] = jnp.zeros_like(blocks)
        blocks[pl.ds(block_shift, rows), :] = dot(
            gathered[rows_of(pair), :], walkers_ref[...], (((1,), (0,)), ((), ()))
        ).astype(jnp.bfloat16)
        core_here = core_ref[:, pl.ds(block_base, window)].astype(jnp.float32)
        trial_there = trial_ref[pl.ds(block_base, window), :]
        for walker in range(walker_count):
            cols = slice(walker * occupied, (walker + 1) * occupied)
            ahead_dot = dot(orbit_own[:, cols], trial_there, CONTRACT_LAST)
            back_dot = dot(trial_ref[own_here, :], blocks[:, cols], CONTRACT_LAST)
            product = core_here * ahead_dot * back_dot
            sums[walker] += weight * jnp.sum(product.reshape(rows // 8, 8, window), axis=0)

    @pl.loop(0, 2 * far + 1)
    def _(task):
        hop = task // 2
        same = lax.rem(task, 2) == 0
        ahead, behind = device(ring + hop, core_id), device(ring - hop, core_id)
        ahead_side, behind_side = device(ring + hop, 1 - core_id), device(ring - hop, 1 - core_id)
        last = hop == far
        middle = jnp.logical_and(hop > 0, hop < far)

        @pl.when(jnp.logical_and(same, middle))
        def _():
            arrived(behind)

            @pl.when(hop < far - 1)
            def _():
                forward(behind, None, right_sems.at[hop], right)

            @pl.when(hop == far - 1)
            def _():
                forward(behind, 0, right_sems.at[hop], right)

            forward(behind, None, side_sems.at[0, hop], partner)
            arrived(ahead)

            @pl.when(hop < far - 1)
            def _():
                forward(ahead, None, left_sems.at[hop], left)

            @pl.when(hop == far - 1)
            def _():
                forward(ahead, 1, left_sems.at[hop], left)

            forward(ahead, None, side_sems.at[1, hop], partner)

        @pl.when(last)
        def _():
            for part in range(2):
                arrived(ahead, part)
                forward(ahead, part, side_sems.at[part, hop], partner)
            for part in range(2):
                arrived(ahead_side, part)

        @pl.when(jnp.logical_not(same))
        def _():
            arrived(ahead_side)

            @pl.when(hop > 0)
            def _():
                arrived(behind_side)

        near = jnp.where(same, ahead, ahead_side)
        pair = jnp.where(jnp.logical_and(last, ring >= far), ahead_side, near)
        exchange(pair, jnp.where(hop == 0, 1.0, 2.0))

        @pl.when(task == 1)
        def _():
            from_everyone(lambda peer: dens_own, dens_slots, dens_sems)
            dens_full[...] = jnp.zeros_like(dens_full)
            for index in range(n):
                there = pl.ds(index * rows // LANES * LANES, window)
                dens_full[:, there] += dens_slots[index].astype(jnp.float32)
            potential = dot(dens_full[...].astype(jnp.bfloat16), core_ref[...], CONTRACT_LAST)[:walker_count]
            field = FIELD_STEP * (node_lookup(draws_ref[...]) - FIELD_STEP * potential)
            hartree = jnp.sum(density_t[:walker_count] * potential, axis=1, keepdims=True)
            energy_own[...] = jnp.zeros_like(energy_own)
            energy_own[:walker_count, :] = jnp.broadcast_to(hartree, (walker_count, LANES))
            field_own[...] = jnp.zeros_like(field_own)
            field_own[:walker_count, :rows] = field
            turned = pltpu.roll(field_own[...], shift, 1)
            for line in range(walker_count):
                fields[line] = turned[line : line + 1]
            to_everyone(lambda peer: fields.at[pl.ds(peer * own // occupied, span)], field_slots, field_sems)
            field_slots[me] = fields[pl.ds(start // occupied, span)]

    walker_exchange = jnp.sum(jnp.sum(sums[...], axis=1), axis=1, keepdims=True)
    energy_own[:walker_count, :] = (energy_own[:walker_count, :] - walker_exchange / occupied) / (2.0 * points)
    energy_slots[me] = energy_own[...]
    to_everyone(lambda peer: energy_own, energy_slots, energy_sems)
    from_everyone(lambda peer: fields.at[pl.ds(peer * own // occupied, span)], field_slots, field_sems)
    chosen[...] = jnp.zeros_like(chosen)
    for index in range(n):
        there = pl.ds(index * rows // LANES * LANES, window)
        for line in range(span):
            chosen[line, :, there] += field_slots[index, line]

    piece = next(p for p in (1280, 640, 256, points) if points % p == 0)
    owner = (start + lax.broadcasted_iota(jnp.int32, (own, 1), 0)) // occupied - start // occupied
    for degree in range(1, TAYLOR + 1):
        if degree > 1:
            total[...] = jnp.zeros_like(total)

        @pl.loop(0, points // piece)
        def _(number):
            here = pl.ds(pl.multiple_of(number * piece, piece), piece)
            block = gathered[here, :]
            current = dot(term[...], block, CONTRACT_LAST).astype(jnp.bfloat16).astype(jnp.float32)
            spread = chosen[0, :, here]
            for line in range(1, span):
                spread = jnp.where(owner == line, chosen[line, :, here], spread)
            scaled = (spread * current).astype(jnp.bfloat16)
            total[...] += dot(scaled, block, (((1,), (0,)), ((), ())))

        term[...] = (total[...] / degree).astype(jnp.bfloat16)
        running = running + term[...].astype(jnp.float32)

    picked = dot(pick[...], running.astype(jnp.bfloat16), CONTRACT_LAST)
    height = outgoing.shape[1]
    for index in range(n):
        outgoing[index, :, :own] = picked[index * height : (index + 1) * height].astype(jnp.bfloat16)
    to_everyone(lambda peer: outgoing.at[peer], incoming, out_sems)
    incoming[me] = outgoing[me]
    from_everyone(lambda peer: energy_own, energy_slots, energy_sems)
    energy = energy_slots[0]
    for index in range(1, n):
        energy = energy + energy_slots[index]
    energy_ref[...] = energy
    from_everyone(lambda peer: outgoing.at[peer], incoming, out_sems)
    out_lane = lax.broadcasted_iota(jnp.int32, (height, LANES), 1)
    for number in range(columns // LANES):
        tile = jnp.zeros((height, LANES), jnp.float32)
        for index in range(n):
            offset = index * own - number * LANES
            if -own < offset < LANES:
                moved = incoming[index].astype(jnp.float32)
                if offset % LANES:
                    moved = pltpu.roll(moved, offset % LANES, 1)
                keep = jnp.logical_and(out_lane >= offset, out_lane < offset + own)
                tile = jnp.where(keep, moved, tile)
        out_ref[:, number * LANES : (number + 1) * LANES] = tile[:own_rows].astype(jnp.bfloat16)

    all_sent(lambda peer: dens_own, dens_slots, dens_sems)
    all_sent(lambda peer: fields.at[pl.ds(peer * own // occupied, span)], field_slots, field_sems)
    all_sent(lambda peer: energy_own, energy_slots, energy_sems)
    all_sent(lambda peer: outgoing.at[peer], incoming, out_sems)
    for hop in range(far):
        for number, (sems, target) in enumerate(((right_sems, right), (left_sems, left))):
            part = number if hop == far - 1 and hop > 0 else None
            send(me, part, sems.at[hop], target).wait_send()
    send(me, None, side_sems.at[0, 0], partner).wait_send()
    for hop in range(1, far + 1):
        for number in range(2):
            part = number if hop == far else None
            send(me, part, side_sems.at[number, hop], partner).wait_send()


def fused(n, points_map, trial, core, flat_walkers, draws_t, walker_count):
    rows, orbitals = points_map.shape
    points, occupied = trial.shape
    columns = flat_walkers.shape[1]
    own, own_rows = columns // n, orbitals // n
    lines = (walker_count + 1 + 15) // 16 * 16
    span = (own + occupied - 2) // occupied + 1
    height = (own_rows + 15) // 16 * 16
    window = (rows + (LANES - 16) + LANES - 1) // LANES * LANES
    full = (points - rows) // LANES * LANES + window
    far = n // 4
    dma = pltpu.SemaphoreType.DMA
    vmem = pltpu.VMEM
    return pl.pallas_call(
        functools.partial(fused_kernel, n, walker_count),
        out_shape=(
            jax.ShapeDtypeStruct((own_rows, columns), jnp.bfloat16),
            jax.ShapeDtypeStruct((lines, LANES), jnp.float32),
        ),
        in_specs=[pl.BlockSpec(memory_space=pl.ANY)] * 4 + [pl.BlockSpec(memory_space=pltpu.VMEM)],
        out_specs=[pl.BlockSpec(memory_space=pltpu.VMEM)] * 2,
        scratch_shapes=[
            vmem((points, orbitals), jnp.bfloat16),
            vmem((points, occupied), jnp.bfloat16),
            vmem((rows, points), jnp.bfloat16),
            vmem((orbitals, columns), jnp.bfloat16),
            vmem((rows, columns), jnp.bfloat16),
            vmem((window, columns), jnp.bfloat16),
            vmem((walker_count, 8, window), jnp.float32),
            vmem((own, orbitals), jnp.float32),
            vmem((own, orbitals), jnp.bfloat16),
            vmem((lines, window), jnp.bfloat16),
            vmem((n, lines, window), jnp.bfloat16),
            vmem((lines, full), jnp.float32),
            vmem((lines, window), jnp.float32),
            vmem((n, span, 1, window), jnp.float32),
            vmem((lines, 1, window), jnp.float32),
            vmem((span, 1, full), jnp.float32),
            vmem((lines, LANES), jnp.float32),
            vmem((n, lines, LANES), jnp.float32),
            vmem((n * height, orbitals), jnp.bfloat16),
            vmem((n, height, LANES), jnp.bfloat16),
            vmem((n, height, LANES), jnp.bfloat16),
            dma((4,)),
            dma((far,)),
            dma((far,)),
            dma((2, far + 1)),
            dma((n, 2)),
            dma((2, n)),
            dma((2, n)),
            dma((2, n)),
            dma((2, n)),
        ],
        compiler_params=pltpu.CompilerParams(
            collective_id=0, has_side_effects=True, vmem_limit_bytes=60 * 2**20
        ),
        name="fused",
    )(points_map, trial, core, flat_walkers, draws_t)


def propagate_kernel(n, occupied, piece, map_ref, field_ref, cols_ref, out_ref, wide, total, term):
    points, orbitals = map_ref.shape
    own = cols_ref.shape[0]
    start = lax.axis_index("pts") * own
    walker_ids = (start + lax.broadcasted_iota(jnp.int32, (1, own), 1)) // occupied
    low = start // occupied
    span = (own + occupied - 2) // occupied + 1
    running = cols_ref[...].astype(jnp.float32)
    term[...] = cols_ref[...]
    for degree in range(1, TAYLOR + 1):
        total[...] = jnp.zeros_like(total)

        @pl.loop(0, points // piece)
        def _(number):
            here = pl.ds(pl.multiple_of(number * piece, piece), piece)
            if degree == 1:
                field = field_ref[here, :]
                lane = lax.broadcasted_iota(jnp.int32, field.shape, 1)
                spread = jnp.zeros((piece, own), jnp.float32)
                for offset in range(span):
                    column = jnp.sum(jnp.where(lane == low + offset, field, 0.0), axis=1, keepdims=True)
                    spread = jnp.where(walker_ids == low + offset, column, spread)
                wide[here, :] = spread
            block = map_ref[here, :]
            current = dot(block, term[...], CONTRACT_LAST).astype(jnp.bfloat16)
            scaled = (wide[here, :] * current.astype(jnp.float32)).astype(jnp.bfloat16)
            total[...] += dot(scaled, block, CONTRACT_FIRST)

        term[...] = (total[...] / degree).astype(jnp.bfloat16)
        running = running + term[...].astype(jnp.float32)
    out_ref[...] = running.astype(jnp.bfloat16)


def propagate(n, occupied, map_full, field_full, own_cols_t):
    points, orbitals = map_full.shape
    own = own_cols_t.shape[0]
    piece = next(p for p in (1280, 640, 256, points // n) if points % p == 0)
    return pl.pallas_call(
        functools.partial(propagate_kernel, n, occupied, piece),
        out_shape=jax.ShapeDtypeStruct((own, orbitals), jnp.bfloat16),
        in_specs=[pl.BlockSpec(memory_space=pltpu.VMEM)] * 3,
        out_specs=pl.BlockSpec(memory_space=pltpu.VMEM),
        scratch_shapes=[
            pltpu.VMEM((points, own), jnp.float32),
            pltpu.VMEM((own, orbitals), jnp.float32),
            pltpu.VMEM((own, orbitals), jnp.bfloat16),
        ],
        cost_estimate=pl.CostEstimate(
            flops=12 * points * orbitals * own, bytes_accessed=2 * map_full.size, transcendentals=0
        ),
        compiler_params=pltpu.CompilerParams(vmem_limit_bytes=60 * 2**20),
        name="propagate",
    )(map_full, field_full, own_cols_t)


def exchange_plain(trial, trial_here, core, orbit):
    core_block = core.astype(jnp.float32)

    def per_walker(operands):
        left_orb, right_orb = operands
        forward = jnp.dot(left_orb, trial.T, preferred_element_type=jnp.float32)
        backward = jnp.dot(trial_here, right_orb.T, preferred_element_type=jnp.float32)
        return jnp.sum(core_block * forward * backward)

    everyone = lax.all_gather(orbit, "pts", axis=0, tiled=True)
    return lax.map(per_walker, (jnp.moveaxis(orbit, 1, 0), jnp.moveaxis(everyone, 1, 0)))


def gather_stacked(part):
    n = lax.axis_size("pts")
    copies = jnp.broadcast_to(part[None], (n,) + part.shape)
    return lax.all_to_all(copies, "pts", split_axis=0, concat_axis=0, tiled=True)


def body(points_map, trial, core, walkers, draws):
    point_rows = points_map.shape[0]
    orbitals = points_map.shape[1]
    walker_count = walkers.shape[1]
    occupied = walkers.shape[2]
    n = lax.axis_size("pts")
    own_rows = orbitals // n
    own_cols = walker_count * occupied // n
    flat_walkers = walkers.reshape(orbitals, walker_count * occupied)
    if point_rows % 16 == 0 and n % 8 == 0 and own_cols <= LANES and occupied == LANES:
        placed, energy = fused(n, points_map, trial, core, flat_walkers, draws.T, walker_count)
        return placed.reshape(own_rows, walker_count, occupied), energy[:walker_count, 0]
    point_first = lax.axis_index("pts") * point_rows
    trial_here = lax.dynamic_slice_in_dim(trial, point_first, point_rows, 0)
    flat_orbit = jnp.dot(points_map, flat_walkers, preferred_element_type=jnp.float32).astype(jnp.bfloat16)
    orbit = flat_orbit.reshape(point_rows, walker_count, occupied)
    density = (
        jnp.sum(orbit.astype(jnp.float32) * trial_here.astype(jnp.float32)[:, None, :], axis=2)
        / math.sqrt(occupied)
    ).astype(jnp.bfloat16)
    potential = jnp.dot(
        core,
        jnp.moveaxis(gather_stacked(density.T), 2, 1).reshape(point_rows * n, walker_count),
        preferred_element_type=jnp.float32,
    )
    field = FIELD_STEP * (node_lookup(draws) - FIELD_STEP * potential)
    field_full = jnp.moveaxis(gather_stacked(field.T), 2, 1).reshape(point_rows * n, walker_count)
    col_start = lax.axis_index("pts") * own_cols
    cols_walkers = lax.dynamic_slice_in_dim(flat_walkers, col_start, own_cols, 1)
    map_full = lax.all_gather(points_map, "pts", axis=0, tiled=True)
    final_t = propagate(n, occupied, map_full, field_full, cols_walkers.T)
    exchange = exchange_plain(trial, trial_here, core, orbit)
    placed = lax.all_to_all(final_t.T, "pts", split_axis=0, concat_axis=1, tiled=True)
    hartree = jnp.sum(density.astype(jnp.float32) * potential, axis=0)
    total_points = point_rows * n
    energy = jnp.sum(gather_stacked((hartree - exchange / occupied) / (2.0 * total_points)), axis=0)
    return (placed.reshape(own_rows, walker_count, occupied), energy)


def solution(mesh):
    placed = (
        P(("mol", "pts"), None),
        P("mol", None),
        P(("mol", "pts"), None),
        P("mol", None, None),
        P(("mol", "pts"), None),
    )
    return jax.shard_map(
        body,
        mesh=mesh,
        in_specs=placed,
        out_specs=(P(("mol", "pts"), None, None), P("mol")),
        check_vma=False,
    )
```

```python
import functools
import math

import jax
import jax.numpy as jnp
from jax import lax
from jax.experimental import pallas as pl
from jax.experimental.pallas import tpu as pltpu
from jax.sharding import PartitionSpec as P

TAYLOR = 3


GAUSS_NODES = (-2.3344142, -0.7419637, 0.7419637, 2.3344142)
FIELD_STEP = 0.15
LANES = 128
CONTRACT_LAST = (((1,), (1,)), ((), ()))
CONTRACT_FIRST = (((0,), (0,)), ((), ()))


def node_lookup(draws):
    values = jnp.zeros(draws.shape, jnp.float32)
    for number, node in enumerate(GAUSS_NODES):
        values = values + jnp.where(draws == number, node, 0.0).astype(jnp.float32)
    return values


def dot(left, right, dims):
    return lax.dot_general(left, right, dims, preferred_element_type=jnp.float32)


def fused_kernel(
    n, walker_count, map_hbm, trial_hbm, core_hbm, walkers_hbm, draws_ref, out_ref, energy_ref,
    gathered, tails, trial_ref, core_ref, walkers_ref, orbit_own, blocks, sums, total, term,
    dens_own, dens_slots, dens_full, field_own, field_slots, fields, chosen, energy_own, energy_slots, pick, outgoing, incoming,
    local_sems, right_sems, left_sems, side_sems, recv_sems, dens_sems, field_sems, energy_sems, out_sems,
):
    rows, columns = orbit_own.shape
    occupied = trial_ref.shape[1]
    own, orbitals = total.shape
    points = gathered.shape[0]
    window = blocks.shape[0]
    own_rows = out_ref.shape[1]
    lines = dens_own.shape[0]
    span = chosen.shape[0]
    chips = n // 2
    far = chips // 2
    top = (rows // 2 + 15) // 16 * 16
    parts = ((0, top), (top, rows - top))
    main = orbitals // LANES * LANES
    rest = orbitals - main
    fold = tails.shape[1]
    me = lax.axis_index("pts")
    core_id = lax.rem(me, 2)
    chip = me // 2
    ring = jnp.where(lax.rem(chip, 2) == 0, chip // 2, chips - 1 - chip // 2)

    def device(place, side):
        place = lax.rem(place + 2 * chips, chips)
        where = jnp.where(place < far, 2 * place, 2 * (chips - 1 - place) + 1)
        return 2 * where + side

    right, left, partner = device(ring + 1, core_id), device(ring - 1, core_id), device(ring, 1 - core_id)

    def rows_of(index):
        return pl.ds(pl.multiple_of(index * rows, 16), rows)

    def slot(index, part):
        if part == 2:
            return tails.at[index]
        offset, length = parts[part]
        return gathered.at[pl.ds(pl.multiple_of(index * rows + offset, 16), length), 0:main]

    def remote(src, dst, send_sem, recv_sem, target):
        return pltpu.make_async_remote_copy(
            src_ref=src,
            dst_ref=dst,
            send_sem=send_sem,
            recv_sem=recv_sem,
            device_id={"pts": target},
            device_id_type=pl.DeviceIdType.MESH,
        )

    def send(index, part, send_sem, target):
        return remote(slot(index, part), slot(index, part), send_sem, recv_sems.at[index, part], target)

    def arrived(index, part):
        send(index, part, side_sems.at[0, 0, 0], partner).wait_recv()

    def unfold(index):
        folded = tails[index].astype(jnp.float32)
        for number, offset in enumerate(range(0, rows, fold)):
            length = min(fold, rows - offset)
            lined = pltpu.roll(folded, LANES - number * rest, 1) if number else folded
            here = pl.ds(pl.multiple_of(index * rows + offset, 16), length)
            gathered[here, main:orbitals] = lined[:length, :rest].astype(jnp.bfloat16)

    def point(hop, chunk):
        ahead, behind = device(ring + hop, core_id), device(ring - hop, core_id)
        messages = ((0,), (1, 2))[chunk]

        @pl.when(hop < far)
        def _():
            for message in messages:
                arrived(behind, message)

                @pl.when(jnp.logical_or(hop < far - 1, chunk == 0))
                def _():
                    send(behind, message, right_sems.at[hop, message], right).start()

                send(behind, message, side_sems.at[0, hop, message], partner).start()
            for message in messages:
                arrived(ahead, message)

                @pl.when(jnp.logical_or(hop < far - 1, chunk == 1))
                def _():
                    send(ahead, message, left_sems.at[hop, message], left).start()

                send(ahead, message, side_sems.at[1, hop, message], partner).start()
            if chunk == 1:
                unfold(behind)
                unfold(ahead)

        @pl.when(hop == far)
        def _():
            for message in messages:
                arrived(ahead, message)
                send(ahead, message, side_sems.at[0, hop, message], partner).start()
            if chunk == 1:
                unfold(ahead)

    def to_everyone(source, slots, sems):
        for step in range(1, n):
            peer = lax.rem(me + step, n)
            remote(source(peer), slots.at[me], sems.at[0, step], sems.at[1, me], peer).start()

    def from_everyone(source, slots, sems):
        for step in range(1, n):
            peer = lax.rem(me + step, n)
            remote(source(peer), slots.at[peer], sems.at[0, step], sems.at[1, peer], peer).wait_recv()

    def all_sent(source, slots, sems):
        for step in range(1, n):
            peer = lax.rem(me + step, n)
            remote(source(peer), slots.at[me], sems.at[0, step], sems.at[1, me], peer).wait_send()

    own_here = rows_of(me)
    local = [
        pltpu.make_async_copy(map_hbm, gathered.at[own_here, :], local_sems.at[0]),
        pltpu.make_async_copy(trial_hbm, trial_ref, local_sems.at[1]),
        pltpu.make_async_copy(core_hbm, core_ref, local_sems.at[2]),
    ]
    local[0].start()
    slabs = [
        pltpu.make_async_copy(
            walkers_hbm.at[walker],
            walkers_ref.at[:, walker * occupied : (walker + 1) * occupied],
            local_sems.at[3 + walker],
        )
        for walker in range(walker_count)
    ]
    barrier = pltpu.get_barrier_semaphore()
    for step in range(1, n):
        pl.semaphore_signal(
            barrier, inc=1, device_id={"pts": lax.rem(me + step, n)}, device_id_type=pl.DeviceIdType.MESH
        )
    for copy in slabs + local[1:]:
        copy.start()
    sums[...] = jnp.zeros_like(sums)
    total[...] = jnp.zeros_like(total)
    local[0].wait()
    pl.semaphore_wait(barrier, n - 1)
    send(me, 0, right_sems.at[0, 0], right).start()
    send(me, 0, left_sems.at[0, 0], left).start()
    send(me, 0, side_sems.at[0, 0, 0], partner).start()
    folded = jnp.zeros((fold, LANES), jnp.float32)
    for number, offset in enumerate(range(0, rows, fold)):
        length = min(fold, rows - offset)
        place = (
            lax.broadcasted_iota(jnp.int32, (rest, LANES), 0) + number * rest
            == lax.broadcasted_iota(jnp.int32, (rest, LANES), 1)
        ).astype(jnp.bfloat16)
        here = pl.ds(pl.multiple_of(me * rows + offset, 16), length)
        lined = dot(gathered[here, main:orbitals], place, (((1,), (0,)), ((), ())))
        if length < fold:
            lined = jnp.concatenate([lined, jnp.zeros((fold - length, LANES), jnp.float32)], axis=0)
        folded = folded + lined
    tails[me] = folded.astype(jnp.bfloat16)

    for copy in slabs:
        copy.wait()
    local[1].wait()
    orbit_own[...] = dot(gathered[own_here, :], walkers_ref[...], (((1,), (0,)), ((), ()))).astype(jnp.bfloat16)
    trial_own = trial_ref[own_here, :].astype(jnp.float32)
    lane = lax.broadcasted_iota(jnp.int32, (rows, LANES), 1)
    density = jnp.zeros((rows, LANES), jnp.float32)
    for walker in range(walker_count):
        cols = slice(walker * occupied, (walker + 1) * occupied)
        column = jnp.sum(orbit_own[:, cols].astype(jnp.float32) * trial_own, axis=1, keepdims=True)
        density = jnp.where(lane == walker, column, density)
    density = (density / math.sqrt(occupied)).astype(jnp.bfloat16)
    unit = (
        lax.broadcasted_iota(jnp.int32, (lines, LANES), 0) == lax.broadcasted_iota(jnp.int32, (lines, LANES), 1)
    ).astype(jnp.bfloat16)
    density_t = dot(unit, density, CONTRACT_LAST)

    def placed(index):
        return pl.multiple_of(index * rows // LANES * LANES, LANES), lax.rem(index * rows, LANES)

    base, shift = placed(me)
    field_own[...] = jnp.zeros_like(field_own)
    field_own[:, :rows] = density_t
    shifted = pltpu.roll(field_own[...], shift, 1).astype(jnp.bfloat16)
    dens_own[...] = shifted
    dens_slots[me] = shifted
    to_everyone(lambda peer: dens_own, dens_slots, dens_sems)
    for message in (1, 2):
        send(me, message, right_sems.at[0, message], right).start()
        send(me, message, left_sems.at[0, message], left).start()
        send(me, message, side_sems.at[0, 0, message], partner).start()

    start = me * own
    left_col = pl.multiple_of(jnp.minimum(start // LANES * LANES, columns - 2 * LANES), LANES)
    choose = (
        lax.broadcasted_iota(jnp.int32, (own, 2 * LANES), 0) + (start - left_col)
        == lax.broadcasted_iota(jnp.int32, (own, 2 * LANES), 1)
    ).astype(jnp.bfloat16)
    cols_own = dot(choose, walkers_ref[:, pl.ds(left_col, 2 * LANES)], CONTRACT_LAST).astype(jnp.bfloat16)
    term[...] = cols_own
    running = cols_own.astype(jnp.float32)
    out_line = lax.broadcasted_iota(jnp.int32, pick.shape, 0)
    out_row = lax.rem(out_line, outgoing.shape[1])
    wanted = jnp.where(out_row < own_rows, out_line // outgoing.shape[1] * own_rows + out_row, -1)
    pick[...] = (wanted == lax.broadcasted_iota(jnp.int32, pick.shape, 1)).astype(jnp.bfloat16)
    local[2].wait()

    def exchange(pair, weight):
        first = pair * rows
        block_base, block_shift = placed(pair)
        block_shift = pl.multiple_of(block_shift, 16)
        blocks[...] = jnp.zeros_like(blocks)
        blocks[pl.ds(block_shift, rows), :] = dot(
            gathered[rows_of(pair), :], walkers_ref[...], (((1,), (0,)), ((), ()))
        ).astype(jnp.bfloat16)
        core_here = core_ref[:, pl.ds(block_base, window)].astype(jnp.float32)
        trial_there = trial_ref[pl.ds(block_base, window), :]
        for walker in range(walker_count):
            cols = slice(walker * occupied, (walker + 1) * occupied)
            ahead_dot = dot(orbit_own[:, cols], trial_there, CONTRACT_LAST)
            back_dot = dot(trial_ref[own_here, :], blocks[:, cols], CONTRACT_LAST)
            product = core_here * ahead_dot * back_dot
            sums[walker] += weight * jnp.sum(product.reshape(rows // 8, 8, window), axis=0)

    owner = (start + lax.broadcasted_iota(jnp.int32, (own, 1), 0)) // occupied - start // occupied

    def take_fields():
        from_everyone(lambda peer: fields.at[pl.ds(peer * own // occupied, span)], field_slots, field_sems)
        chosen[...] = jnp.zeros_like(chosen)
        for index in range(n):
            there = pl.ds(index * rows // LANES * LANES, window)
            for line in range(span):
                chosen[line, :, there] += field_slots[index, line]

    def add_chip(where):
        for side in range(2):
            index = 2 * where + side
            block = gathered[rows_of(index), :]
            current = dot(term[...], block, CONTRACT_LAST).astype(jnp.bfloat16).astype(jnp.float32)
            turn = lax.rem(window - lax.rem(index * rows, LANES), window)
            lined = [pltpu.roll(field_slots[index, line], turn, 1)[:, :rows] for line in range(span)]
            spread = lined[0]
            for line in range(1, span):
                spread = jnp.where(owner == line, lined[line], spread)
            scaled = (spread * current).astype(jnp.bfloat16)
            total[...] += dot(scaled, block, (((1,), (0,)), ((), ())))

    @pl.loop(0, 2 * far + 1)
    def _(task):
        hop = task // 2
        same = lax.rem(task, 2) == 0
        last = hop == far

        @pl.when(jnp.logical_not(same))
        def _():
            point(hop + 1, 0)

        @pl.when(jnp.logical_and(same, task > 0))
        def _():
            point(hop, 1)

        ahead, ahead_side = device(ring + hop, core_id), device(ring + hop, 1 - core_id)
        behind_side = device(ring - hop, 1 - core_id)

        @pl.when(jnp.logical_or(jnp.logical_not(same), last))
        def _():
            for message in range(3):
                arrived(ahead_side, message)
            unfold(ahead_side)

            @pl.when(jnp.logical_and(hop > 0, hop < far))
            def _():
                for message in range(3):
                    arrived(behind_side, message)
                unfold(behind_side)

        near = jnp.where(same, ahead, ahead_side)
        pair = jnp.where(jnp.logical_and(last, ring >= far), ahead_side, near)
        exchange(pair, jnp.where(hop == 0, 1.0, 2.0))

        @pl.when(task == far)
        def _():
            take_fields()

        @pl.when(task >= far)
        def _():
            late = task - far
            away = (late + 1) // 2
            add_chip(device(jnp.where(lax.rem(late, 2) == 1, ring + away, ring - away), 0) // 2)

        @pl.when(task == 1)
        def _():
            from_everyone(lambda peer: dens_own, dens_slots, dens_sems)
            dens_full[...] = jnp.zeros_like(dens_full)
            for index in range(n):
                there = pl.ds(index * rows // LANES * LANES, window)
                dens_full[:, there] += dens_slots[index].astype(jnp.float32)
            potential = dot(dens_full[...].astype(jnp.bfloat16), core_ref[...], CONTRACT_LAST)[:walker_count]
            field = FIELD_STEP * (node_lookup(draws_ref[...]) - FIELD_STEP * potential)
            hartree = jnp.sum(density_t[:walker_count] * potential, axis=1, keepdims=True)
            energy_own[...] = jnp.zeros_like(energy_own)
            energy_own[:walker_count, :] = jnp.broadcast_to(hartree, (walker_count, LANES))
            field_own[...] = jnp.zeros_like(field_own)
            field_own[:walker_count, :rows] = field
            turned = pltpu.roll(field_own[...], shift, 1)
            for line in range(walker_count):
                fields[line] = turned[line : line + 1]
            to_everyone(lambda peer: fields.at[pl.ds(peer * own // occupied, span)], field_slots, field_sems)
            field_slots[me] = fields[pl.ds(start // occupied, span)]

    walker_exchange = jnp.sum(jnp.sum(sums[...], axis=1), axis=1, keepdims=True)
    energy_own[:walker_count, :] = (energy_own[:walker_count, :] - walker_exchange / occupied) / (2.0 * points)
    energy_slots[me] = energy_own[...]
    to_everyone(lambda peer: energy_own, energy_slots, energy_sems)
    @pl.loop(far + 1, 2 * far)
    def _(late):
        away = (late + 1) // 2
        add_chip(device(jnp.where(lax.rem(late, 2) == 1, ring + away, ring - away), 0) // 2)

    term[...] = total[...].astype(jnp.bfloat16)
    running = running + term[...].astype(jnp.float32)
    piece = next(p for p in (1280, 640, 256, points) if points % p == 0)
    for degree in range(2, TAYLOR + 1):
        total[...] = jnp.zeros_like(total)

        @pl.loop(0, points // piece)
        def _(number):
            here = pl.ds(pl.multiple_of(number * piece, piece), piece)
            block = gathered[here, :]
            current = dot(term[...], block, CONTRACT_LAST).astype(jnp.bfloat16).astype(jnp.float32)
            spread = chosen[0, :, here]
            for line in range(1, span):
                spread = jnp.where(owner == line, chosen[line, :, here], spread)
            scaled = (spread * current).astype(jnp.bfloat16)
            total[...] += dot(scaled, block, (((1,), (0,)), ((), ())))

        term[...] = (total[...] / degree).astype(jnp.bfloat16)
        running = running + term[...].astype(jnp.float32)

    picked = dot(pick[...], running.astype(jnp.bfloat16), CONTRACT_LAST)
    height = outgoing.shape[1]
    for index in range(n):
        outgoing[index, :, :own] = picked[index * height : (index + 1) * height].astype(jnp.bfloat16)
    to_everyone(lambda peer: outgoing.at[peer], incoming, out_sems)
    incoming[me] = outgoing[me]
    from_everyone(lambda peer: energy_own, energy_slots, energy_sems)
    energy = energy_slots[0]
    for index in range(1, n):
        energy = energy + energy_slots[index]
    energy_ref[...] = energy
    from_everyone(lambda peer: outgoing.at[peer], incoming, out_sems)
    out_lane = lax.broadcasted_iota(jnp.int32, (height, LANES), 1)
    for number in range(columns // LANES):
        tile = jnp.zeros((height, LANES), jnp.float32)
        for index in range(n):
            offset = index * own - number * LANES
            if -own < offset < LANES:
                moved = incoming[index].astype(jnp.float32)
                if offset % LANES:
                    moved = pltpu.roll(moved, offset % LANES, 1)
                keep = jnp.logical_and(out_lane >= offset, out_lane < offset + own)
                tile = jnp.where(keep, moved, tile)
        out_ref[number] = tile[:own_rows].astype(jnp.bfloat16)

    all_sent(lambda peer: dens_own, dens_slots, dens_sems)
    all_sent(lambda peer: fields.at[pl.ds(peer * own // occupied, span)], field_slots, field_sems)
    all_sent(lambda peer: energy_own, energy_slots, energy_sems)
    all_sent(lambda peer: outgoing.at[peer], incoming, out_sems)
    for hop in range(far):
        for number, (sems, target) in enumerate(((right_sems, right), (left_sems, left))):
            for message in range(3) if hop < far - 1 else ((0,), (1, 2))[number]:
                send(me, message, sems.at[hop, message], target).wait_send()
    for hop in range(far + 1):
        for number in range(2 if 0 < hop < far else 1):
            for message in range(3):
                send(me, message, side_sems.at[number, hop, message], partner).wait_send()


def fused(n, points_map, trial, core, walker_major, draws_t):
    rows, orbitals = points_map.shape
    points, occupied = trial.shape
    walker_count = walker_major.shape[0]
    columns = walker_count * occupied
    fold = (rows // (LANES // (orbitals % LANES)) + 15) // 16 * 16
    own, own_rows = columns // n, orbitals // n
    lines = (walker_count + 1 + 15) // 16 * 16
    span = (own + occupied - 2) // occupied + 1
    height = (own_rows + 15) // 16 * 16
    window = (rows + (LANES - 16) + LANES - 1) // LANES * LANES
    full = (points - rows) // LANES * LANES + window
    far = n // 4
    dma = pltpu.SemaphoreType.DMA
    vmem = pltpu.VMEM
    return pl.pallas_call(
        functools.partial(fused_kernel, n, walker_count),
        out_shape=(
            jax.ShapeDtypeStruct((walker_count, own_rows, occupied), jnp.bfloat16),
            jax.ShapeDtypeStruct((lines, LANES), jnp.float32),
        ),
        in_specs=[pl.BlockSpec(memory_space=pl.ANY)] * 4 + [pl.BlockSpec(memory_space=pltpu.VMEM)],
        out_specs=[pl.BlockSpec(memory_space=pltpu.VMEM)] * 2,
        scratch_shapes=[
            vmem((points, orbitals), jnp.bfloat16),
            vmem((n, fold, LANES), jnp.bfloat16),
            vmem((points, occupied), jnp.bfloat16),
            vmem((rows, points), jnp.bfloat16),
            vmem((orbitals, columns), jnp.bfloat16),
            vmem((rows, columns), jnp.bfloat16),
            vmem((window, columns), jnp.bfloat16),
            vmem((walker_count, 8, window), jnp.float32),
            vmem((own, orbitals), jnp.float32),
            vmem((own, orbitals), jnp.bfloat16),
            vmem((lines, window), jnp.bfloat16),
            vmem((n, lines, window), jnp.bfloat16),
            vmem((lines, full), jnp.float32),
            vmem((lines, window), jnp.float32),
            vmem((n, span, 1, window), jnp.float32),
            vmem((lines, 1, window), jnp.float32),
            vmem((span, 1, full), jnp.float32),
            vmem((lines, LANES), jnp.float32),
            vmem((n, lines, LANES), jnp.float32),
            vmem((n * height, orbitals), jnp.bfloat16),
            vmem((n, height, LANES), jnp.bfloat16),
            vmem((n, height, LANES), jnp.bfloat16),
            dma((3 + walker_count,)),
            dma((far, 3)),
            dma((far, 3)),
            dma((2, far + 1, 3)),
            dma((n, 3)),
            dma((2, n)),
            dma((2, n)),
            dma((2, n)),
            dma((2, n)),
        ],
        compiler_params=pltpu.CompilerParams(
            collective_id=0, has_side_effects=True, vmem_limit_bytes=60 * 2**20
        ),
        name="fused",
    )(points_map, trial, core, walker_major, draws_t)


def propagate_kernel(n, occupied, piece, map_ref, field_ref, cols_ref, out_ref, wide, total, term):
    points, orbitals = map_ref.shape
    own = cols_ref.shape[0]
    start = lax.axis_index("pts") * own
    walker_ids = (start + lax.broadcasted_iota(jnp.int32, (1, own), 1)) // occupied
    low = start // occupied
    span = (own + occupied - 2) // occupied + 1
    running = cols_ref[...].astype(jnp.float32)
    term[...] = cols_ref[...]
    for degree in range(1, TAYLOR + 1):
        total[...] = jnp.zeros_like(total)

        @pl.loop(0, points // piece)
        def _(number):
            here = pl.ds(pl.multiple_of(number * piece, piece), piece)
            if degree == 1:
                field = field_ref[here, :]
                lane = lax.broadcasted_iota(jnp.int32, field.shape, 1)
                spread = jnp.zeros((piece, own), jnp.float32)
                for offset in range(span):
                    column = jnp.sum(jnp.where(lane == low + offset, field, 0.0), axis=1, keepdims=True)
                    spread = jnp.where(walker_ids == low + offset, column, spread)
                wide[here, :] = spread
            block = map_ref[here, :]
            current = dot(block, term[...], CONTRACT_LAST).astype(jnp.bfloat16)
            scaled = (wide[here, :] * current.astype(jnp.float32)).astype(jnp.bfloat16)
            total[...] += dot(scaled, block, CONTRACT_FIRST)

        term[...] = (total[...] / degree).astype(jnp.bfloat16)
        running = running + term[...].astype(jnp.float32)
    out_ref[...] = running.astype(jnp.bfloat16)


def propagate(n, occupied, map_full, field_full, own_cols_t):
    points, orbitals = map_full.shape
    own = own_cols_t.shape[0]
    piece = next(p for p in (1280, 640, 256, points // n) if points % p == 0)
    return pl.pallas_call(
        functools.partial(propagate_kernel, n, occupied, piece),
        out_shape=jax.ShapeDtypeStruct((own, orbitals), jnp.bfloat16),
        in_specs=[pl.BlockSpec(memory_space=pltpu.VMEM)] * 3,
        out_specs=pl.BlockSpec(memory_space=pltpu.VMEM),
        scratch_shapes=[
            pltpu.VMEM((points, own), jnp.float32),
            pltpu.VMEM((own, orbitals), jnp.float32),
            pltpu.VMEM((own, orbitals), jnp.bfloat16),
        ],
        cost_estimate=pl.CostEstimate(
            flops=12 * points * orbitals * own, bytes_accessed=2 * map_full.size, transcendentals=0
        ),
        compiler_params=pltpu.CompilerParams(vmem_limit_bytes=60 * 2**20),
        name="propagate",
    )(map_full, field_full, own_cols_t)


def exchange_plain(trial, trial_here, core, orbit):
    core_block = core.astype(jnp.float32)

    def per_walker(operands):
        left_orb, right_orb = operands
        forward = jnp.dot(left_orb, trial.T, preferred_element_type=jnp.float32)
        backward = jnp.dot(trial_here, right_orb.T, preferred_element_type=jnp.float32)
        return jnp.sum(core_block * forward * backward)

    everyone = lax.all_gather(orbit, "pts", axis=0, tiled=True)
    return lax.map(per_walker, (jnp.moveaxis(orbit, 1, 0), jnp.moveaxis(everyone, 1, 0)))


def gather_stacked(part):
    n = lax.axis_size("pts")
    copies = jnp.broadcast_to(part[None], (n,) + part.shape)
    return lax.all_to_all(copies, "pts", split_axis=0, concat_axis=0, tiled=True)


def body(points_map, trial, core, walkers, draws):
    point_rows = points_map.shape[0]
    orbitals = points_map.shape[1]
    walker_count = walkers.shape[1]
    occupied = walkers.shape[2]
    n = lax.axis_size("pts")
    own_rows = orbitals // n
    own_cols = walker_count * occupied // n
    rest = orbitals % LANES
    if point_rows % 16 == 0 and n % 8 == 0 and own_cols <= LANES and occupied == LANES and rest and LANES % rest == 0:
        placed, energy = fused(n, points_map, trial, core, jnp.moveaxis(walkers, 1, 0), draws.T)
        return jnp.moveaxis(placed, 0, 1), energy[:walker_count, 0]
    flat_walkers = walkers.reshape(orbitals, walker_count * occupied)
    point_first = lax.axis_index("pts") * point_rows
    trial_here = lax.dynamic_slice_in_dim(trial, point_first, point_rows, 0)
    flat_orbit = jnp.dot(points_map, flat_walkers, preferred_element_type=jnp.float32).astype(jnp.bfloat16)
    orbit = flat_orbit.reshape(point_rows, walker_count, occupied)
    density = (
        jnp.sum(orbit.astype(jnp.float32) * trial_here.astype(jnp.float32)[:, None, :], axis=2)
        / math.sqrt(occupied)
    ).astype(jnp.bfloat16)
    potential = jnp.dot(
        core,
        jnp.moveaxis(gather_stacked(density.T), 2, 1).reshape(point_rows * n, walker_count),
        preferred_element_type=jnp.float32,
    )
    field = FIELD_STEP * (node_lookup(draws) - FIELD_STEP * potential)
    field_full = jnp.moveaxis(gather_stacked(field.T), 2, 1).reshape(point_rows * n, walker_count)
    col_start = lax.axis_index("pts") * own_cols
    cols_walkers = lax.dynamic_slice_in_dim(flat_walkers, col_start, own_cols, 1)
    map_full = lax.all_gather(points_map, "pts", axis=0, tiled=True)
    final_t = propagate(n, occupied, map_full, field_full, cols_walkers.T)
    exchange = exchange_plain(trial, trial_here, core, orbit)
    placed = lax.all_to_all(final_t.T, "pts", split_axis=0, concat_axis=1, tiled=True)
    hartree = jnp.sum(density.astype(jnp.float32) * potential, axis=0)
    total_points = point_rows * n
    energy = jnp.sum(gather_stacked((hartree - exchange / occupied) / (2.0 * total_points)), axis=0)
    return (placed.reshape(own_rows, walker_count, occupied), energy)


def solution(mesh):
    placed = (
        P(("mol", "pts"), None),
        P("mol", None),
        P(("mol", "pts"), None),
        P("mol", None, None),
        P(("mol", "pts"), None),
    )
    return jax.shard_map(
        body,
        mesh=mesh,
        in_specs=placed,
        out_specs=(P(("mol", "pts"), None, None), P("mol")),
        check_vma=False,
    )
```

```python
import functools
import math

import jax
import jax.numpy as jnp
from jax import lax
from jax.experimental import pallas as pl
from jax.experimental.pallas import tpu as pltpu
from jax.sharding import PartitionSpec as P

TAYLOR = 3


GAUSS_NODES = (-2.3344142, -0.7419637, 0.7419637, 2.3344142)
FIELD_STEP = 0.15
LANES = 128
CONTRACT_LAST = (((1,), (1,)), ((), ()))
CONTRACT_FIRST = (((0,), (0,)), ((), ()))


def node_lookup(draws):
    values = jnp.zeros(draws.shape, jnp.float32)
    for number, node in enumerate(GAUSS_NODES):
        values = values + jnp.where(draws == number, node, 0.0).astype(jnp.float32)
    return values


def dot(left, right, dims):
    return lax.dot_general(left, right, dims, preferred_element_type=jnp.float32)


def fused_kernel(
    n, walker_count, map_hbm, trial_hbm, core_hbm, walkers_hbm, draws_ref, out_ref, energy_ref,
    gathered, tails, trial_ref, core_ref, walkers_ref, orbit_own, blocks, sums, total, term,
    dens_own, dens_slots, dens_full, field_own, field_slots, fields, chosen, energy_own, energy_slots, pick, outgoing, incoming,
    local_sems, in_sems, out_sems_map, across_sems, side_sems, recv_sems, dens_sems, field_sems, energy_sems, out_sems,
):
    rows, columns = orbit_own.shape
    occupied = trial_ref.shape[1]
    own, orbitals = total.shape
    points = gathered.shape[0]
    window = blocks.shape[0]
    own_rows = out_ref.shape[1]
    half = LANES // 2
    height = pick.shape[0] // n
    lines = dens_own.shape[0]
    span = chosen.shape[0]
    chips = n // 2
    far = chips // 2
    top = (rows // 2 + 15) // 16 * 16
    parts = ((0, top), (top, rows - top))
    main = orbitals // LANES * LANES
    rest = orbitals - main
    fold = tails.shape[1]
    me = lax.axis_index("pts")
    core_id = lax.rem(me, 2)
    chip = me // 2
    ring = jnp.where(lax.rem(chip, 2) == 0, chip // 2, chips - 1 - chip // 2)

    def device(place, side):
        place = lax.rem(place + 2 * chips, chips)
        where = jnp.where(place < far, 2 * place, 2 * (chips - 1 - place) + 1)
        return 2 * where + side

    quarter = lax.rem(ring, 4)
    is_middle = jnp.logical_or(quarter == 1, quarter == 2)
    is_corner = jnp.logical_not(is_middle)
    sign = jnp.where(quarter < 2, 1, -1)
    steps = (0, sign, -sign, 2 * sign, -2 * sign, 3 * sign, far, -3 * sign)
    inner, outer = device(ring + sign, core_id), device(ring - sign, core_id)
    across, partner = device(chips - 1 - ring, core_id), device(ring, 1 - core_id)

    def near(which, side):
        return device(ring + steps[which], side)

    def share(which):
        other = lax.rem(ring + steps[which] + 2 * chips, chips)
        return device(other, jnp.where(ring < other, core_id, 1 - core_id))

    def rows_of(index):
        return pl.ds(pl.multiple_of(index * rows, 16), rows)

    def slot(index, part):
        if part == 2:
            return tails.at[index]
        offset, length = parts[part]
        return gathered.at[pl.ds(pl.multiple_of(index * rows + offset, 16), length), 0:main]

    def remote(src, dst, send_sem, recv_sem, target):
        return pltpu.make_async_remote_copy(
            src_ref=src,
            dst_ref=dst,
            send_sem=send_sem,
            recv_sem=recv_sem,
            device_id={"pts": target},
            device_id_type=pl.DeviceIdType.MESH,
        )

    def send(index, part, send_sem, target):
        return remote(slot(index, part), slot(index, part), send_sem, recv_sems.at[index, part], target)

    def arrived(index, part):
        send(index, part, side_sems.at[0, 0], partner).wait_recv()

    def unfold(index):
        folded = tails[index].astype(jnp.float32)
        for number, offset in enumerate(range(0, rows, fold)):
            length = min(fold, rows - offset)
            lined = pltpu.roll(folded, LANES - number * rest, 1) if number else folded
            here = pl.ds(pl.multiple_of(index * rows + offset, 16), length)
            gathered[here, main:orbitals] = lined[:length, :rest].astype(jnp.bfloat16)

    def go(which, message, sems, number, target):
        send(near(which, core_id), message, sems.at[number, message], target).start()

    def land(which, message):
        arrived(near(which, core_id), message)
        go(which, message, side_sems, which, partner)

    def point(stage, chunk):
        messages = ((0,), (1, 2))[chunk]
        if stage == 1:
            for message in messages:
                land(1, message)
                go(1, message, out_sems_map, 1, outer)
                land(2, message)
                go(2, message, in_sems, 1, inner)

                @pl.when(is_middle)
                def _():
                    go(1, message, across_sems, 1, across)
                    land(7, message)

            if chunk == 1:
                unfold(near(1, core_id))
                unfold(near(2, core_id))

                @pl.when(is_middle)
                def _():
                    unfold(near(7, core_id))

        if stage == 2:
            for message in messages:
                land(3, message)
                go(3, message, out_sems_map, 2, outer)
                land(4, message)

                @pl.when(is_middle)
                def _():
                    if chunk == 0:
                        go(4, message, in_sems, 2, inner)
                    else:
                        go(3, message, across_sems, 2, across)
                    land(6, message)

            if chunk == 1:
                unfold(near(3, core_id))
                unfold(near(4, core_id))

                @pl.when(is_middle)
                def _():
                    unfold(near(6, core_id))

        if stage == 3:
            for message in messages:
                land(5, message)

                @pl.when(is_corner)
                def _():
                    go(5, message, out_sems_map, 3, outer)
                    land(7, message)

            if chunk == 1:
                unfold(near(5, core_id))

                @pl.when(is_corner)
                def _():
                    unfold(near(7, core_id))

        if stage == 4:
            for message in messages:
                land(6, message)
            if chunk == 1:
                unfold(near(6, core_id))

    def land_side(which):
        index = near(which, 1 - core_id)
        for message in range(3):
            arrived(index, message)
        unfold(index)

    def to_everyone(source, slots, sems):
        for step in range(1, n):
            peer = lax.rem(me + step, n)
            remote(source(peer), slots.at[me], sems.at[0, step], sems.at[1, me], peer).start()

    def from_everyone(source, slots, sems):
        for step in range(1, n):
            peer = lax.rem(me + step, n)
            remote(source(peer), slots.at[peer], sems.at[0, step], sems.at[1, peer], peer).wait_recv()

    def all_sent(source, slots, sems):
        for step in range(1, n):
            peer = lax.rem(me + step, n)
            remote(source(peer), slots.at[me], sems.at[0, step], sems.at[1, me], peer).wait_send()

    middle_first = n // 4

    def low_of(number):
        return number * own // occupied

    def each_middle(act):
        for number in range(n // 2):

            @pl.when(me != middle_first + number)
            def _():
                act(number, middle_first + number)

    def field_send(number, peer):
        return remote(
            fields.at[pl.ds(low_of(number), span)], field_slots.at[me], field_sems.at[0, number],
            field_sems.at[1, me], peer,
        )

    own_here = rows_of(me)
    local = [
        pltpu.make_async_copy(map_hbm, gathered.at[own_here, :], local_sems.at[0]),
        pltpu.make_async_copy(trial_hbm, trial_ref, local_sems.at[1]),
        pltpu.make_async_copy(core_hbm, core_ref, local_sems.at[2]),
    ]
    local[0].start()
    slabs = [
        pltpu.make_async_copy(
            walkers_hbm.at[walker],
            walkers_ref.at[:, walker * occupied : (walker + 1) * occupied],
            local_sems.at[3 + walker],
        )
        for walker in range(walker_count)
    ]
    barrier = pltpu.get_barrier_semaphore()
    for step in range(1, n):
        pl.semaphore_signal(
            barrier, inc=1, device_id={"pts": lax.rem(me + step, n)}, device_id_type=pl.DeviceIdType.MESH
        )
    for copy in slabs + local[1:]:
        copy.start()
    sums[...] = jnp.zeros_like(sums)
    total[...] = jnp.zeros_like(total)
    local[0].wait()
    pl.semaphore_wait(barrier, n - 1)
    def start_own(message):
        go(0, message, in_sems, 0, inner)
        go(0, message, out_sems_map, 0, outer)

        @pl.when(is_middle)
        def _():
            go(0, message, across_sems, 0, across)

        go(0, message, side_sems, 0, partner)

    start_own(0)
    folded = jnp.zeros((fold, LANES), jnp.float32)
    for number, offset in enumerate(range(0, rows, fold)):
        length = min(fold, rows - offset)
        place = (
            lax.broadcasted_iota(jnp.int32, (rest, LANES), 0) + number * rest
            == lax.broadcasted_iota(jnp.int32, (rest, LANES), 1)
        ).astype(jnp.bfloat16)
        here = pl.ds(pl.multiple_of(me * rows + offset, 16), length)
        lined = dot(gathered[here, main:orbitals], place, (((1,), (0,)), ((), ())))
        if length < fold:
            lined = jnp.concatenate([lined, jnp.zeros((fold - length, LANES), jnp.float32)], axis=0)
        folded = folded + lined
    tails[me] = folded.astype(jnp.bfloat16)

    for copy in slabs:
        copy.wait()
    local[1].wait()
    orbit_own[...] = dot(gathered[own_here, :], walkers_ref[...], (((1,), (0,)), ((), ()))).astype(jnp.bfloat16)
    trial_own = trial_ref[own_here, :].astype(jnp.float32)
    lane = lax.broadcasted_iota(jnp.int32, (rows, LANES), 1)
    density = jnp.zeros((rows, LANES), jnp.float32)
    for walker in range(walker_count):
        cols = slice(walker * occupied, (walker + 1) * occupied)
        column = jnp.sum(orbit_own[:, cols].astype(jnp.float32) * trial_own, axis=1, keepdims=True)
        density = jnp.where(lane == walker, column, density)
    density = (density / math.sqrt(occupied)).astype(jnp.bfloat16)
    unit = (
        lax.broadcasted_iota(jnp.int32, (lines, LANES), 0) == lax.broadcasted_iota(jnp.int32, (lines, LANES), 1)
    ).astype(jnp.bfloat16)
    density_t = dot(unit, density, CONTRACT_LAST)

    def placed(index):
        return pl.multiple_of(index * rows // LANES * LANES, LANES), lax.rem(index * rows, LANES)

    base, shift = placed(me)
    field_own[...] = jnp.zeros_like(field_own)
    field_own[:, :rows] = density_t
    shifted = pltpu.roll(field_own[...], shift, 1).astype(jnp.bfloat16)
    dens_own[...] = shifted
    dens_slots[me] = shifted
    to_everyone(lambda peer: dens_own, dens_slots, dens_sems)
    for message in (1, 2):
        start_own(message)

    mine = jnp.clip(me - middle_first, 0, n // 2 - 1)
    start = mine * own
    left_col = pl.multiple_of(jnp.minimum(start // LANES * LANES, columns - 2 * LANES), LANES)
    choose = (
        lax.broadcasted_iota(jnp.int32, (own, 2 * LANES), 0) + (start - left_col)
        == lax.broadcasted_iota(jnp.int32, (own, 2 * LANES), 1)
    ).astype(jnp.bfloat16)
    cols_own = dot(choose, walkers_ref[:, pl.ds(left_col, 2 * LANES)], CONTRACT_LAST).astype(jnp.bfloat16)
    term[...] = cols_own
    out_line = lax.broadcasted_iota(jnp.int32, pick.shape, 0)
    out_row = lax.rem(out_line, height)
    wanted = jnp.where(out_row < own_rows, out_line // height * own_rows + out_row, -1)
    pick[...] = (wanted == lax.broadcasted_iota(jnp.int32, pick.shape, 1)).astype(jnp.bfloat16)
    local[2].wait()

    def exchange(pair, weight):
        first = pair * rows
        block_base, block_shift = placed(pair)
        block_shift = pl.multiple_of(block_shift, 16)
        blocks[...] = jnp.zeros_like(blocks)

        @pl.when(pair == me)
        def _():
            blocks[pl.ds(block_shift, rows), :] = orbit_own[...]

        @pl.when(pair != me)
        def _():
            blocks[pl.ds(block_shift, rows), :] = dot(
                gathered[rows_of(pair), :], walkers_ref[...], (((1,), (0,)), ((), ()))
            ).astype(jnp.bfloat16)

        core_here = core_ref[:, pl.ds(block_base, window)].astype(jnp.float32)
        trial_there = trial_ref[pl.ds(block_base, window), :]
        for walker in range(walker_count):
            cols = slice(walker * occupied, (walker + 1) * occupied)
            ahead_dot = dot(orbit_own[:, cols], trial_there, CONTRACT_LAST)
            back_dot = dot(trial_ref[own_here, :], blocks[:, cols], CONTRACT_LAST)
            product = core_here * ahead_dot * back_dot
            sums[walker] += weight * jnp.sum(product.reshape(rows // 8, 8, window), axis=0)

    owner = (start + lax.broadcasted_iota(jnp.int32, (own, 1), 0)) // occupied - start // occupied

    def take_fields():
        for step in range(1, n):
            peer = lax.rem(me + step, n)
            remote(
                fields.at[pl.ds(0, span)], field_slots.at[peer], field_sems.at[0, 0], field_sems.at[1, peer], peer
            ).wait_recv()
        chosen[...] = jnp.zeros_like(chosen)
        for index in range(n):
            there = pl.ds(index * rows // LANES * LANES, window)
            for line in range(span):
                chosen[line, :, there] += field_slots[index, line]

    def add_chip(which):
        where = near(which, 0) // 2
        for side in range(2):
            index = 2 * where + side
            block = gathered[rows_of(index), :]
            current = dot(term[...], block, CONTRACT_LAST).astype(jnp.bfloat16).astype(jnp.float32)
            turn = lax.rem(window - lax.rem(index * rows, LANES), window)
            lined = [pltpu.roll(field_slots[index, line], turn, 1)[:, :rows] for line in range(span)]
            spread = lined[0]
            for line in range(1, span):
                spread = jnp.where(owner == line, lined[line], spread)
            scaled = (spread * current).astype(jnp.bfloat16)
            total[...] += dot(scaled, block, (((1,), (0,)), ((), ())))

    corner_list = (
        me, partner, near(1, core_id), near(1, 1 - core_id), share(2), near(3, core_id), near(3, 1 - core_id),
        near(4, core_id), near(4, 1 - core_id), near(7, core_id), near(7, 1 - core_id), share(5), share(6),
    )
    middle_list = {0: me, 1: partner, 3: share(1), 4: share(7), 7: share(6)}
    stops = {1: (1, 0), 2: (1, 1), 4: (2, 0), 5: (2, 1), 8: (3, 0), 9: (3, 1)}
    corner_stops = {11: (4, 0), 12: (4, 1)}
    sides = {1: ((0,), ()), 3: ((1, 2), (7,)), 6: ((3, 4), (6,)), 10: ((5,), ())}
    corner_sides = {10: (7,), 12: (6,)}
    adds = {5: (0, 1), 6: (2, 7), 8: (3, 4, 6)}

    @pl.loop(0, len(corner_list))
    def _(task):
        for number, (stage, chunk) in stops.items():

            @pl.when(task == number)
            def _():
                point(stage, chunk)

        for number, (stage, chunk) in corner_stops.items():

            @pl.when(jnp.logical_and(task == number, is_corner))
            def _():
                point(stage, chunk)

        for number, (both, middle) in sides.items():

            @pl.when(task == number)
            def _():
                for which in both:
                    land_side(which)

                @pl.when(is_middle)
                def _():
                    for which in middle:
                        land_side(which)

        for number, those in corner_sides.items():

            @pl.when(jnp.logical_and(task == number, is_corner))
            def _():
                for which in those:
                    land_side(which)

        pair = me
        active = is_corner
        for number, choice in enumerate(corner_list):
            pair = jnp.where(task == number, choice, pair)
        for number, choice in middle_list.items():
            hit = jnp.logical_and(task == number, is_middle)
            pair = jnp.where(hit, choice, pair)
            active = jnp.logical_or(active, hit)

        @pl.when(active)
        def _():
            exchange(pair, jnp.where(task < 2, 1.0, 2.0))

        @pl.when(task == 2)
        def _():
            from_everyone(lambda peer: dens_own, dens_slots, dens_sems)
            dens_full[...] = jnp.zeros_like(dens_full)
            for index in range(n):
                there = pl.ds(index * rows // LANES * LANES, window)
                dens_full[:, there] += dens_slots[index].astype(jnp.float32)
            potential = dot(dens_full[...].astype(jnp.bfloat16), core_ref[...], CONTRACT_LAST)[:walker_count]
            field = FIELD_STEP * (node_lookup(draws_ref[...]) - FIELD_STEP * potential)
            hartree = jnp.sum(density_t[:walker_count] * potential, axis=1, keepdims=True)
            energy_own[...] = jnp.zeros_like(energy_own)
            energy_own[:walker_count, :] = jnp.broadcast_to(hartree, (walker_count, LANES))
            field_own[...] = jnp.zeros_like(field_own)
            field_own[:walker_count, :rows] = field
            turned = pltpu.roll(field_own[...], shift, 1)
            for line in range(walker_count):
                fields[line] = turned[line : line + 1]
            each_middle(lambda number, peer: field_send(number, peer).start())
            field_slots[me] = fields[pl.ds(start // occupied, span)]

        @pl.when(jnp.logical_and(task == 5, is_middle))
        def _():
            take_fields()

        for number, those in adds.items():

            @pl.when(jnp.logical_and(task == number, is_middle))
            def _():
                for which in those:
                    add_chip(which)


    walker_exchange = jnp.sum(jnp.sum(sums[...], axis=1), axis=1, keepdims=True)
    energy_own[:walker_count, :] = (energy_own[:walker_count, :] - walker_exchange / occupied) / (2.0 * points)
    energy_slots[me] = energy_own[...]
    to_everyone(lambda peer: energy_own, energy_slots, energy_sems)
    piece = next(p for p in (1280, 640, 256, points) if points % p == 0)

    @pl.when(is_middle)
    def _():
        add_chip(5)
        running = term[...].astype(jnp.float32)
        term[...] = total[...].astype(jnp.bfloat16)
        running = running + term[...].astype(jnp.float32)
        for degree in range(2, TAYLOR + 1):
            total[...] = jnp.zeros_like(total)

            @pl.loop(0, points // piece)
            def _(number):
                here = pl.ds(pl.multiple_of(number * piece, piece), piece)
                block = gathered[here, :]
                current = dot(term[...], block, CONTRACT_LAST).astype(jnp.bfloat16).astype(jnp.float32)
                spread = chosen[0, :, here]
                for line in range(1, span):
                    spread = jnp.where(owner == line, chosen[line, :, here], spread)
                scaled = (spread * current).astype(jnp.bfloat16)
                total[...] += dot(scaled, block, (((1,), (0,)), ((), ())))

            term[...] = (total[...] / degree).astype(jnp.bfloat16)
            running = running + term[...].astype(jnp.float32)
        final = running.astype(jnp.bfloat16)
        first = dot(pick[...], final[:LANES], CONTRACT_LAST)
        padded = jnp.concatenate([final[LANES:], jnp.zeros((half, orbitals), jnp.bfloat16)], axis=0)
        second = dot(pick[...], padded, CONTRACT_LAST)
        for index in range(n):
            upper = second[index * height : index * height + height // 2]
            lower = second[index * height + height // 2 : (index + 1) * height]
            outgoing[index, :height] = first[index * height : (index + 1) * height].astype(jnp.bfloat16)
            outgoing[index, height:] = (upper + pltpu.roll(lower, half, 1)).astype(jnp.bfloat16)
        for step in range(1, n):
            peer = lax.rem(me + step, n)
            remote(outgoing.at[peer], incoming.at[mine], out_sems.at[0, step], out_sems.at[1, mine], peer).start()
        incoming[mine] = outgoing[me]

    from_everyone(lambda peer: energy_own, energy_slots, energy_sems)
    energy = energy_slots[0]
    for index in range(1, n):
        energy = energy + energy_slots[index]
    energy_ref[...] = energy
    each_middle(
        lambda number, peer: remote(
            outgoing.at[0], incoming.at[number], out_sems.at[0, 0], out_sems.at[1, number], peer
        ).wait_recv()
    )
    out_lane = lax.broadcasted_iota(jnp.int32, (height, LANES), 1)
    pieces = []
    for number in range(n // 2):
        got = incoming[number].astype(jnp.float32)
        top_part, low_part = got[:height], got[height:]
        pieces.append((top_part, 0))
        pieces.append((top_part, 1))
        pieces.append((jnp.concatenate([low_part, pltpu.roll(low_part, half, 1)], axis=0), 0))
    for number in range(walker_count):
        (low, low_at), (high, high_at) = pieces[2 * number], pieces[2 * number + 1]
        low = pltpu.roll(low, half, 1) if low_at == 1 else low
        high = pltpu.roll(high, half, 1) if high_at == 0 else high
        out_ref[number] = jnp.where(out_lane < half, low, high)[:own_rows].astype(jnp.bfloat16)

    all_sent(lambda peer: dens_own, dens_slots, dens_sems)
    all_sent(lambda peer: energy_own, energy_slots, energy_sems)
    each_middle(lambda number, peer: field_send(number, peer).wait_send())

    def sent(sems, number, messages, target):
        for message in messages:
            send(me, message, sems.at[number, message], target).wait_send()

    for number in range(2):
        sent(in_sems, number, range(3), inner)
    for number in range(3):
        sent(out_sems_map, number, range(3), outer)
    for number in range(7):
        sent(side_sems, number, range(3), partner)
    sent(side_sems, 7, range(3), partner)

    @pl.when(is_middle)
    def _():
        sent(in_sems, 2, (0,), inner)
        sent(across_sems, 0, range(3), across)
        sent(across_sems, 1, range(3), across)
        sent(across_sems, 2, (1, 2), across)
        for step in range(1, n):
            peer = lax.rem(me + step, n)
            remote(
                outgoing.at[peer], incoming.at[mine], out_sems.at[0, step], out_sems.at[1, mine], peer
            ).wait_send()

    @pl.when(is_corner)
    def _():
        sent(out_sems_map, 3, range(3), outer)


def fused(n, points_map, trial, core, walker_major, draws_t):
    rows, orbitals = points_map.shape
    points, occupied = trial.shape
    walker_count = walker_major.shape[0]
    columns = walker_count * occupied
    fold = (rows // (LANES // (orbitals % LANES)) + 15) // 16 * 16
    own, own_rows = columns // (n // 2), orbitals // n
    lines = (walker_count + 1 + 15) // 16 * 16
    span = max((k * own + own - 1) // occupied - k * own // occupied + 1 for k in range(n // 2))
    height = (own_rows + 31) // 32 * 32
    window = (rows + (LANES - 16) + LANES - 1) // LANES * LANES
    full = (points - rows) // LANES * LANES + window
    far = n // 4
    dma = pltpu.SemaphoreType.DMA
    vmem = pltpu.VMEM
    return pl.pallas_call(
        functools.partial(fused_kernel, n, walker_count),
        out_shape=(
            jax.ShapeDtypeStruct((walker_count, own_rows, occupied), jnp.bfloat16),
            jax.ShapeDtypeStruct((lines, LANES), jnp.float32),
        ),
        in_specs=[pl.BlockSpec(memory_space=pl.ANY)] * 4 + [pl.BlockSpec(memory_space=pltpu.VMEM)],
        out_specs=[pl.BlockSpec(memory_space=pltpu.VMEM)] * 2,
        scratch_shapes=[
            vmem((points, orbitals), jnp.bfloat16),
            vmem((n, fold, LANES), jnp.bfloat16),
            vmem((points, occupied), jnp.bfloat16),
            vmem((rows, points), jnp.bfloat16),
            vmem((orbitals, columns), jnp.bfloat16),
            vmem((rows, columns), jnp.bfloat16),
            vmem((window, columns), jnp.bfloat16),
            vmem((walker_count, 8, window), jnp.float32),
            vmem((own, orbitals), jnp.float32),
            vmem((own, orbitals), jnp.bfloat16),
            vmem((lines, window), jnp.bfloat16),
            vmem((n, lines, window), jnp.bfloat16),
            vmem((lines, full), jnp.float32),
            vmem((lines, window), jnp.float32),
            vmem((n, span, 1, window), jnp.float32),
            vmem((lines, 1, window), jnp.float32),
            vmem((span, 1, full), jnp.float32),
            vmem((lines, LANES), jnp.float32),
            vmem((n, lines, LANES), jnp.float32),
            vmem((n * height, orbitals), jnp.bfloat16),
            vmem((n, height + height // 2, LANES), jnp.bfloat16),
            vmem((n // 2, height + height // 2, LANES), jnp.bfloat16),
            dma((3 + walker_count,)),
            dma((3, 3)),
            dma((4, 3)),
            dma((3, 3)),
            dma((8, 3)),
            dma((n, 3)),
            dma((2, n)),
            dma((2, n)),
            dma((2, n)),
            dma((2, n)),
        ],
        compiler_params=pltpu.CompilerParams(
            collective_id=0, has_side_effects=True, vmem_limit_bytes=60 * 2**20
        ),
        name="fused",
    )(points_map, trial, core, walker_major, draws_t)


def propagate_kernel(n, occupied, piece, map_ref, field_ref, cols_ref, out_ref, wide, total, term):
    points, orbitals = map_ref.shape
    own = cols_ref.shape[0]
    start = lax.axis_index("pts") * own
    walker_ids = (start + lax.broadcasted_iota(jnp.int32, (1, own), 1)) // occupied
    low = start // occupied
    span = (own + occupied - 2) // occupied + 1
    running = cols_ref[...].astype(jnp.float32)
    term[...] = cols_ref[...]
    for degree in range(1, TAYLOR + 1):
        total[...] = jnp.zeros_like(total)

        @pl.loop(0, points // piece)
        def _(number):
            here = pl.ds(pl.multiple_of(number * piece, piece), piece)
            if degree == 1:
                field = field_ref[here, :]
                lane = lax.broadcasted_iota(jnp.int32, field.shape, 1)
                spread = jnp.zeros((piece, own), jnp.float32)
                for offset in range(span):
                    column = jnp.sum(jnp.where(lane == low + offset, field, 0.0), axis=1, keepdims=True)
                    spread = jnp.where(walker_ids == low + offset, column, spread)
                wide[here, :] = spread
            block = map_ref[here, :]
            current = dot(block, term[...], CONTRACT_LAST).astype(jnp.bfloat16)
            scaled = (wide[here, :] * current.astype(jnp.float32)).astype(jnp.bfloat16)
            total[...] += dot(scaled, block, CONTRACT_FIRST)

        term[...] = (total[...] / degree).astype(jnp.bfloat16)
        running = running + term[...].astype(jnp.float32)
    out_ref[...] = running.astype(jnp.bfloat16)


def propagate(n, occupied, map_full, field_full, own_cols_t):
    points, orbitals = map_full.shape
    own = own_cols_t.shape[0]
    piece = next(p for p in (1280, 640, 256, points // n) if points % p == 0)
    return pl.pallas_call(
        functools.partial(propagate_kernel, n, occupied, piece),
        out_shape=jax.ShapeDtypeStruct((own, orbitals), jnp.bfloat16),
        in_specs=[pl.BlockSpec(memory_space=pltpu.VMEM)] * 3,
        out_specs=pl.BlockSpec(memory_space=pltpu.VMEM),
        scratch_shapes=[
            pltpu.VMEM((points, own), jnp.float32),
            pltpu.VMEM((own, orbitals), jnp.float32),
            pltpu.VMEM((own, orbitals), jnp.bfloat16),
        ],
        cost_estimate=pl.CostEstimate(
            flops=12 * points * orbitals * own, bytes_accessed=2 * map_full.size, transcendentals=0
        ),
        compiler_params=pltpu.CompilerParams(vmem_limit_bytes=60 * 2**20),
        name="propagate",
    )(map_full, field_full, own_cols_t)


def exchange_plain(trial, trial_here, core, orbit):
    core_block = core.astype(jnp.float32)

    def per_walker(operands):
        left_orb, right_orb = operands
        forward = jnp.dot(left_orb, trial.T, preferred_element_type=jnp.float32)
        backward = jnp.dot(trial_here, right_orb.T, preferred_element_type=jnp.float32)
        return jnp.sum(core_block * forward * backward)

    everyone = lax.all_gather(orbit, "pts", axis=0, tiled=True)
    return lax.map(per_walker, (jnp.moveaxis(orbit, 1, 0), jnp.moveaxis(everyone, 1, 0)))


def gather_stacked(part):
    n = lax.axis_size("pts")
    copies = jnp.broadcast_to(part[None], (n,) + part.shape)
    return lax.all_to_all(copies, "pts", split_axis=0, concat_axis=0, tiled=True)


def body(points_map, trial, core, walkers, draws):
    point_rows = points_map.shape[0]
    orbitals = points_map.shape[1]
    walker_count = walkers.shape[1]
    occupied = walkers.shape[2]
    n = lax.axis_size("pts")
    own_rows = orbitals // n
    own_cols = walker_count * occupied // n
    rest = orbitals % LANES
    if point_rows % 16 == 0 and n == 16 and 4 * own_cols == 3 * LANES and occupied == LANES and rest and LANES % rest == 0:
        placed, energy = fused(n, points_map, trial, core, jnp.moveaxis(walkers, 1, 0), draws.T)
        return jnp.moveaxis(placed, 0, 1), energy[:walker_count, 0]
    flat_walkers = walkers.reshape(orbitals, walker_count * occupied)
    point_first = lax.axis_index("pts") * point_rows
    trial_here = lax.dynamic_slice_in_dim(trial, point_first, point_rows, 0)
    flat_orbit = jnp.dot(points_map, flat_walkers, preferred_element_type=jnp.float32).astype(jnp.bfloat16)
    orbit = flat_orbit.reshape(point_rows, walker_count, occupied)
    density = (
        jnp.sum(orbit.astype(jnp.float32) * trial_here.astype(jnp.float32)[:, None, :], axis=2)
        / math.sqrt(occupied)
    ).astype(jnp.bfloat16)
    potential = jnp.dot(
        core,
        jnp.moveaxis(gather_stacked(density.T), 2, 1).reshape(point_rows * n, walker_count),
        preferred_element_type=jnp.float32,
    )
    field = FIELD_STEP * (node_lookup(draws) - FIELD_STEP * potential)
    field_full = jnp.moveaxis(gather_stacked(field.T), 2, 1).reshape(point_rows * n, walker_count)
    col_start = lax.axis_index("pts") * own_cols
    cols_walkers = lax.dynamic_slice_in_dim(flat_walkers, col_start, own_cols, 1)
    map_full = lax.all_gather(points_map, "pts", axis=0, tiled=True)
    final_t = propagate(n, occupied, map_full, field_full, cols_walkers.T)
    exchange = exchange_plain(trial, trial_here, core, orbit)
    placed = lax.all_to_all(final_t.T, "pts", split_axis=0, concat_axis=1, tiled=True)
    hartree = jnp.sum(density.astype(jnp.float32) * potential, axis=0)
    total_points = point_rows * n
    energy = jnp.sum(gather_stacked((hartree - exchange / occupied) / (2.0 * total_points)), axis=0)
    return (placed.reshape(own_rows, walker_count, occupied), energy)


def solution(mesh):
    placed = (
        P(("mol", "pts"), None),
        P("mol", None),
        P(("mol", "pts"), None),
        P("mol", None, None),
        P(("mol", "pts"), None),
    )
    return jax.shard_map(
        body,
        mesh=mesh,
        in_specs=placed,
        out_specs=(P(("mol", "pts"), None, None), P("mol")),
        check_vma=False,
    )
```

```python
import functools
import math

import jax
import jax.numpy as jnp
from jax import lax
from jax.experimental import pallas as pl
from jax.experimental.pallas import tpu as pltpu
from jax.sharding import PartitionSpec as P

TAYLOR = 3


GAUSS_NODES = (-2.3344142, -0.7419637, 0.7419637, 2.3344142)
FIELD_STEP = 0.15
LANES = 128
CONTRACT_LAST = (((1,), (1,)), ((), ()))
CONTRACT_FIRST = (((0,), (0,)), ((), ()))


def node_lookup(draws):
    values = jnp.zeros(draws.shape, jnp.float32)
    for number, node in enumerate(GAUSS_NODES):
        values = values + jnp.where(draws == number, node, 0.0).astype(jnp.float32)
    return values


def dot(left, right, dims):
    return lax.dot_general(left, right, dims, preferred_element_type=jnp.float32)


def fused_kernel(
    n, walker_count, own, map_hbm, trial_hbm, core_hbm, walkers_hbm, draws_ref, out_ref, energy_ref,
    gathered, tails, trial_ref, core_ref, walkers_ref, orbit_own, blocks, sums, turned_map, gram, shared_gram, whole_half, shared_half,
    dens_own, dens_slots, dens_full, field_own, field_slots, fields, energy_own, energy_slots, pick, outgoing, incoming,
    local_sems, in_sems, out_sems_map, across_sems, side_sems, recv_sems, dens_sems, field_sems, energy_sems, out_sems, gram_sems,
):
    rows, columns = orbit_own.shape
    occupied = trial_ref.shape[1]
    orbitals = gram.shape[0]
    points = gathered.shape[0]
    window = blocks.shape[0]
    own_rows = out_ref.shape[1]
    half = LANES // 2
    height = pick.shape[0] // n
    lines = dens_own.shape[0]
    span = field_slots.shape[1]
    width = 2 * LANES
    split = (orbitals // LANES * LANES) - width
    chips = n // 2
    far = chips // 2
    top = (rows // 2 + 15) // 16 * 16
    parts = ((0, top), (top, rows - top))
    main = orbitals // LANES * LANES
    rest = orbitals - main
    fold = tails.shape[1]
    me = lax.axis_index("pts")
    core_id = lax.rem(me, 2)
    chip = me // 2
    ring = jnp.where(lax.rem(chip, 2) == 0, chip // 2, chips - 1 - chip // 2)

    def device(place, side):
        place = lax.rem(place + 2 * chips, chips)
        where = jnp.where(place < far, 2 * place, 2 * (chips - 1 - place) + 1)
        return 2 * where + side

    quarter = lax.rem(ring, 4)
    is_middle = jnp.logical_or(quarter == 1, quarter == 2)
    is_corner = jnp.logical_not(is_middle)
    sign = jnp.where(quarter < 2, 1, -1)
    steps = (0, sign, -sign, 2 * sign, -2 * sign, 3 * sign, far, -3 * sign)
    inner, outer = device(ring + sign, core_id), device(ring - sign, core_id)
    across, partner = device(chips - 1 - ring, core_id), device(ring, 1 - core_id)

    def near(which, side):
        return device(ring + steps[which], side)

    def share(which):
        other = lax.rem(ring + steps[which] + 2 * chips, chips)
        return device(other, jnp.where(ring < other, core_id, 1 - core_id))

    def rows_of(index):
        return pl.ds(pl.multiple_of(index * rows, 16), rows)

    def slot(index, part):
        if part == 2:
            return tails.at[index]
        offset, length = parts[part]
        return gathered.at[pl.ds(pl.multiple_of(index * rows + offset, 16), length), 0:main]

    def remote(src, dst, send_sem, recv_sem, target):
        return pltpu.make_async_remote_copy(
            src_ref=src,
            dst_ref=dst,
            send_sem=send_sem,
            recv_sem=recv_sem,
            device_id={"pts": target},
            device_id_type=pl.DeviceIdType.MESH,
        )

    def send(index, part, send_sem, target):
        return remote(slot(index, part), slot(index, part), send_sem, recv_sems.at[index, part], target)

    def arrived(index, part):
        send(index, part, side_sems.at[0, 0], partner).wait_recv()

    def unfold(index):
        folded = tails[index].astype(jnp.float32)
        for number, offset in enumerate(range(0, rows, fold)):
            length = min(fold, rows - offset)
            lined = pltpu.roll(folded, LANES - number * rest, 1) if number else folded
            here = pl.ds(pl.multiple_of(index * rows + offset, 16), length)
            gathered[here, main:orbitals] = lined[:length, :rest].astype(jnp.bfloat16)

    def go(which, message, sems, number, target):
        send(near(which, core_id), message, sems.at[number, message], target).start()

    def land(which, message):
        arrived(near(which, core_id), message)
        go(which, message, side_sems, which, partner)

    def point(stage, chunk):
        messages = ((0,), (1, 2))[chunk]
        if stage == 1:
            for message in messages:
                land(1, message)
                go(1, message, out_sems_map, 1, outer)
                land(2, message)
                go(2, message, in_sems, 1, inner)

                @pl.when(is_middle)
                def _():
                    go(1, message, across_sems, 1, across)
                    land(7, message)

            if chunk == 1:
                unfold(near(1, core_id))
                unfold(near(2, core_id))

                @pl.when(is_middle)
                def _():
                    unfold(near(7, core_id))

        if stage == 2:
            for message in messages:
                land(3, message)
                go(3, message, out_sems_map, 2, outer)
                land(4, message)

                @pl.when(is_middle)
                def _():
                    if chunk == 0:
                        go(4, message, in_sems, 2, inner)
                    else:
                        go(3, message, across_sems, 2, across)
                    land(6, message)

            if chunk == 1:
                unfold(near(3, core_id))
                unfold(near(4, core_id))

                @pl.when(is_middle)
                def _():
                    unfold(near(6, core_id))

    def far_point(which, chunk, onward):
        for message in ((0,), (1, 2))[chunk]:
            land(which, message)
            if onward:
                go(which, message, out_sems_map, 3, outer)
        if chunk == 1:
            unfold(near(which, core_id))

    def land_side(which):
        index = near(which, 1 - core_id)
        for message in range(3):
            arrived(index, message)
        unfold(index)

    def to_everyone(source, slots, sems):
        for step in range(1, n):
            peer = lax.rem(me + step, n)
            remote(source(peer), slots.at[me], sems.at[0, step], sems.at[1, me], peer).start()

    def from_everyone(source, slots, sems):
        for step in range(1, n):
            peer = lax.rem(me + step, n)
            remote(source(peer), slots.at[peer], sems.at[0, step], sems.at[1, peer], peer).wait_recv()

    def all_sent(source, slots, sems):
        for step in range(1, n):
            peer = lax.rem(me + step, n)
            remote(source(peer), slots.at[me], sems.at[0, step], sems.at[1, me], peer).wait_send()

    middle_first = n // 4

    def low_of(number):
        return number * own // occupied

    def each_middle(act):
        for number in range(n // 2):

            @pl.when(me != middle_first + number)
            def _():
                act(number, middle_first + number)

    def field_send(number, peer):
        return remote(
            fields.at[pl.ds(low_of(number), span)], field_slots.at[me], field_sems.at[0, number],
            field_sems.at[1, me], peer,
        )

    own_here = rows_of(me)
    local = [
        pltpu.make_async_copy(map_hbm, gathered.at[own_here, :], local_sems.at[0]),
        pltpu.make_async_copy(trial_hbm, trial_ref, local_sems.at[1]),
        pltpu.make_async_copy(core_hbm, core_ref, local_sems.at[2]),
    ]
    local[0].start()
    slabs = [
        pltpu.make_async_copy(
            walkers_hbm.at[walker],
            walkers_ref.at[:, walker * occupied : (walker + 1) * occupied],
            local_sems.at[3 + walker],
        )
        for walker in range(walker_count)
    ]
    barrier = pltpu.get_barrier_semaphore()
    for step in range(1, n):
        pl.semaphore_signal(
            barrier, inc=1, device_id={"pts": lax.rem(me + step, n)}, device_id_type=pl.DeviceIdType.MESH
        )
    for copy in slabs + local[1:]:
        copy.start()
    sums[...] = jnp.zeros_like(sums)
    gram[...] = jnp.zeros_like(gram)
    shared_gram[...] = jnp.zeros_like(shared_gram)
    local[0].wait()
    pl.semaphore_wait(barrier, n - 1)
    def start_own(message):
        go(0, message, in_sems, 0, inner)
        go(0, message, out_sems_map, 0, outer)

        @pl.when(is_middle)
        def _():
            go(0, message, across_sems, 0, across)

        go(0, message, side_sems, 0, partner)

    start_own(0)
    folded = jnp.zeros((fold, LANES), jnp.float32)
    for number, offset in enumerate(range(0, rows, fold)):
        length = min(fold, rows - offset)
        place = (
            lax.broadcasted_iota(jnp.int32, (rest, LANES), 0) + number * rest
            == lax.broadcasted_iota(jnp.int32, (rest, LANES), 1)
        ).astype(jnp.bfloat16)
        here = pl.ds(pl.multiple_of(me * rows + offset, 16), length)
        lined = dot(gathered[here, main:orbitals], place, (((1,), (0,)), ((), ())))
        if length < fold:
            lined = jnp.concatenate([lined, jnp.zeros((fold - length, LANES), jnp.float32)], axis=0)
        folded = folded + lined
    tails[me] = folded.astype(jnp.bfloat16)

    for copy in slabs:
        copy.wait()
    local[1].wait()
    orbit_own[...] = dot(gathered[own_here, :], walkers_ref[...], (((1,), (0,)), ((), ()))).astype(jnp.bfloat16)
    trial_own = trial_ref[own_here, :].astype(jnp.float32)
    lane = lax.broadcasted_iota(jnp.int32, (rows, LANES), 1)
    density = jnp.zeros((rows, LANES), jnp.float32)
    for walker in range(walker_count):
        cols = slice(walker * occupied, (walker + 1) * occupied)
        column = jnp.sum(orbit_own[:, cols].astype(jnp.float32) * trial_own, axis=1, keepdims=True)
        density = jnp.where(lane == walker, column, density)
    density = (density / math.sqrt(occupied)).astype(jnp.bfloat16)
    unit = (
        lax.broadcasted_iota(jnp.int32, (lines, LANES), 0) == lax.broadcasted_iota(jnp.int32, (lines, LANES), 1)
    ).astype(jnp.bfloat16)
    density_t = dot(unit, density, CONTRACT_LAST)

    def placed(index):
        return pl.multiple_of(index * rows // LANES * LANES, LANES), lax.rem(index * rows, LANES)

    base, shift = placed(me)
    field_own[...] = jnp.zeros_like(field_own)
    field_own[:, :rows] = density_t
    shifted = pltpu.roll(field_own[...], shift, 1).astype(jnp.bfloat16)
    dens_own[...] = shifted
    dens_slots[me] = shifted
    def dens_out(step):
        peer = partner if step == 1 else lax.rem(me + step, n)
        return remote(dens_own, dens_slots.at[me], dens_sems.at[0, step], dens_sems.at[1, me], peer)

    def dens_relay(step):
        source = lax.rem(me + step, n)
        return remote(
            dens_slots.at[source], dens_slots.at[source], dens_sems.at[0, step + 1], dens_sems.at[1, source], partner
        )

    for step in (*range(2, n, 2), 1):
        dens_out(step).start()
    for message in (1, 2):
        start_own(message)

    mine = jnp.clip(me - middle_first, 0, n // 2 - 1)
    whole = mine // 2 * 3 + 2 * core_id
    shared = mine // 2 * 3 + 1

    def columns_of(walker):
        return walkers_ref[:, pl.ds(pl.multiple_of(walker * occupied, occupied), occupied)]

    def selector(count, offset):
        return (
            lax.broadcasted_iota(jnp.int32, (count, occupied), 0) + offset
            == lax.broadcasted_iota(jnp.int32, (count, occupied), 1)
        ).astype(jnp.bfloat16)

    out_line = lax.broadcasted_iota(jnp.int32, pick.shape, 0)
    out_row = lax.rem(out_line, height)
    wanted = jnp.where(out_row < own_rows, out_line // height * own_rows + out_row, -1)
    pick[...] = (wanted == lax.broadcasted_iota(jnp.int32, pick.shape, 1)).astype(jnp.bfloat16)
    local[2].wait()

    def exchange(pair, weight):
        first = pair * rows
        block_base, block_shift = placed(pair)
        block_shift = pl.multiple_of(block_shift, 16)
        blocks[...] = jnp.zeros_like(blocks)

        @pl.when(pair == me)
        def _():
            blocks[pl.ds(block_shift, rows), :] = orbit_own[...]

        @pl.when(pair != me)
        def _():
            blocks[pl.ds(block_shift, rows), :] = dot(
                gathered[rows_of(pair), :], walkers_ref[...], (((1,), (0,)), ((), ()))
            ).astype(jnp.bfloat16)

        core_here = core_ref[:, pl.ds(block_base, window)].astype(jnp.float32)
        trial_there = trial_ref[pl.ds(block_base, window), :]
        for walker in range(walker_count):
            cols = slice(walker * occupied, (walker + 1) * occupied)
            ahead_dot = dot(orbit_own[:, cols], trial_there, CONTRACT_LAST)
            back_dot = dot(trial_ref[own_here, :], blocks[:, cols], CONTRACT_LAST)
            product = core_here * ahead_dot * back_dot
            sums[walker] += weight * jnp.sum(product.reshape(rows // 8, 8, window), axis=0)

    def take_fields():
        for step in range(1, n):
            peer = lax.rem(me + step, n)
            remote(
                fields.at[pl.ds(0, span)], field_slots.at[peer], field_sems.at[0, 0], field_sems.at[1, peer], peer
            ).wait_recv()

    def add_chip(chip_index):
        here = pl.ds(pl.multiple_of(chip_index * 2 * rows, 16), 2 * rows)
        block = gathered[here, :]
        wide = (2 * rows + LANES - 1) // LANES * LANES
        lined = []
        for line in range(span):
            row = jnp.zeros((1, wide), jnp.float32)
            for side in range(2):
                index = 2 * chip_index + side
                part = jnp.concatenate(
                    [field_slots[index, line], jnp.zeros((1, wide - window), jnp.float32)], axis=1
                )
                turn = lax.rem(side * rows - lax.rem(index * rows, LANES) + wide, wide)
                row = row + pltpu.roll(part, turn, 1)
            lined.append(row[:, : 2 * rows])
        turned_map[...] = jnp.transpose(block)
        whole_field = jnp.where(core_id == 0, lined[0], lined[1])
        shared_field = jnp.where(core_id == 0, lined[1], lined[0])
        plain = (((1,), (0,)), ((), ()))

        def accumulate(target, scaled, firsts):
            for first in firsts:
                cols = slice(first, first + width)
                stop = orbitals if first + width == main else first + width
                target[:stop, cols] += dot(scaled[:stop], block[:, cols], plain)
                if stop < orbitals:
                    target[main:, cols] += dot(scaled[main:], block[:, cols], plain)

        scaled = (turned_map[...].astype(jnp.float32) * whole_field).astype(jnp.bfloat16)
        accumulate(gram, scaled, range(0, main, width))
        gram[main:, main:] += dot(scaled[main:], block[:, main:], plain)
        shared_map = (turned_map[...].astype(jnp.float32) * shared_field).astype(jnp.bfloat16)
        shared_gram[main:, main:] += dot(shared_map[main:], block[:, main:], plain)

        @pl.when(core_id == 0)
        def _():
            accumulate(shared_gram, shared_map, range(split, main, width))

        @pl.when(core_id == 1)
        def _():
            accumulate(shared_gram, shared_map, range(0, split, width))

    corner_list = (
        me, partner, near(1, core_id), near(1, 1 - core_id), share(2), near(3, core_id), near(3, 1 - core_id),
        share(4), near(7, core_id), near(7, 1 - core_id), share(5), share(6),
    )
    middle_list = {0: me, 1: partner, 3: share(1), 4: share(7), 6: share(4), 7: share(6)}
    stops = {1: (1, 0), 2: (1, 1), 4: (2, 0), 5: (2, 1)}
    middle_far = {8: ((5, 0, False),), 9: ((5, 1, False),)}
    corner_far = {
        6: ((5, 0, True),), 7: ((7, 0, False),), 8: ((5, 1, True), (7, 1, False)),
        11: ((6, 0, False), (6, 1, False)),
    }
    middle_sides = {1: (0,), 3: (1, 2, 7), 6: (3, 4, 6), 10: (5,)}
    corner_sides = {1: (0,), 3: (1, 2), 6: (3,), 7: (4,), 9: (7,), 10: (5,), 11: (6,)}
    add_order = (0, 1, 2, 7, 3, 4, 6, 5)
    add_until = {4: 2, 5: 4, 7: 5, 8: 7, 10: 8}

    @pl.loop(0, len(corner_list))
    def _(task):
        @pl.when(task == 1)
        def _():
            for step in range(2, n, 2):
                dens_relay(step).wait_recv()
                dens_relay(step).start()
            for step in range(0, n, 2):
                source = lax.rem(partner + step, n)
                remote(
                    dens_own, dens_slots.at[source], dens_sems.at[0, 0], dens_sems.at[1, source], partner
                ).wait_recv()
            dens_full[...] = jnp.zeros_like(dens_full)
            for index in range(n):
                there = pl.ds(index * rows // LANES * LANES, window)
                dens_full[:, there] += dens_slots[index].astype(jnp.float32)
            potential = dot(dens_full[...].astype(jnp.bfloat16), core_ref[...], CONTRACT_LAST)[:walker_count]
            field = FIELD_STEP * (node_lookup(draws_ref[...]) - FIELD_STEP * potential)
            hartree = jnp.sum(density_t[:walker_count] * potential, axis=1, keepdims=True)
            energy_own[...] = jnp.zeros_like(energy_own)
            energy_own[:walker_count, :] = jnp.broadcast_to(hartree, (walker_count, LANES))
            field_own[...] = jnp.zeros_like(field_own)
            field_own[:walker_count, :rows] = field
            turned = pltpu.roll(field_own[...], shift, 1)
            for line in range(walker_count):
                fields[line] = turned[line : line + 1]
            each_middle(lambda number, peer: field_send(number, peer).start())
            field_slots[me] = fields[pl.ds(mine * own // occupied, span)]

        for number, (stage, chunk) in stops.items():

            @pl.when(task == number)
            def _():
                point(stage, chunk)

        for role, far_stops, side_stops in (
            (is_middle, middle_far, middle_sides), (is_corner, corner_far, corner_sides)
        ):
            for number, those in far_stops.items():

                @pl.when(jnp.logical_and(task == number, role))
                def _():
                    for which, chunk, onward in those:
                        far_point(which, chunk, onward)

            for number, those in side_stops.items():

                @pl.when(jnp.logical_and(task == number, role))
                def _():
                    for which in those:
                        land_side(which)

        pair = me
        active = is_corner
        for number, choice in enumerate(corner_list):
            pair = jnp.where(task == number, choice, pair)
        for number, choice in middle_list.items():
            hit = jnp.logical_and(task == number, is_middle)
            pair = jnp.where(hit, choice, pair)
            active = jnp.logical_or(active, hit)

        @pl.when(active)
        def _():
            exchange(pair, jnp.where(task < 2, 1.0, 2.0))

        @pl.when(jnp.logical_and(task == 4, is_middle))
        def _():
            take_fields()

        add_from, add_to = 0, 0
        done = 0
        for number, until in add_until.items():
            add_from = jnp.where(task == number, done, add_from)
            add_to = jnp.where(task == number, until, add_to)
            done = until

        @pl.loop(jnp.where(is_middle, add_from, 0), jnp.where(is_middle, add_to, 0))
        def _(item):
            place = me
            for number, which in enumerate(add_order):
                place = jnp.where(item == number, near(which, 0), place)
            add_chip(place // 2)

    walker_exchange = jnp.sum(jnp.sum(sums[...], axis=1), axis=1, keepdims=True)
    energy_own[:walker_count, :] = (energy_own[:walker_count, :] - walker_exchange / occupied) / (2.0 * points)
    energy_slots[me] = energy_own[...]
    to_everyone(lambda peer: energy_own, energy_slots, energy_sems)
    def gram_copy(side):
        cols = slice(split, main) if side == 0 else slice(0, split)
        return remote(
            shared_half.at[:, cols], shared_half.at[:, cols], gram_sems.at[0], gram_sems.at[1], partner
        )

    def both_sides(act):
        for side in range(2):

            @pl.when(core_id == side)
            def _():
                act(side)

    def apply(value, matrix):
        parts = []
        for first in range(0, main, width):
            cols = slice(first, first + width)
            part = dot(value[:, : first + width], matrix[: first + width, cols], (((1,), (0,)), ((), ())))
            for later in range(first + width, main, width):
                there = slice(later, later + width)
                part = part + dot(value[:, there], matrix[cols, there], CONTRACT_LAST)
            parts.append(part + dot(value[:, main:], matrix[main:, cols], (((1,), (0,)), ((), ()))))
        last = dot(value[:, :main], matrix[main:, :main], CONTRACT_LAST)
        parts.append(last + dot(value[:, main:], matrix[main:, main:], (((1,), (0,)), ((), ()))))
        return jnp.concatenate(parts, axis=1)

    @pl.when(is_middle)
    def _():
        def pack_shared(side):
            cols = slice(split, main) if side == 0 else slice(0, split)
            shared_half[:, cols] = shared_gram[:, cols].astype(jnp.bfloat16)
            gram_copy(side).start()

        both_sides(pack_shared)
        shared_half[main:, main:] = shared_gram[main:, main:].astype(jnp.bfloat16)
        whole_half[...] = gram[...].astype(jnp.bfloat16)
        whole_term = dot(selector(occupied, 0), columns_of(whole), CONTRACT_LAST).astype(jnp.bfloat16)
        shared_term = dot(selector(half, core_id * half), columns_of(shared), CONTRACT_LAST).astype(jnp.bfloat16)
        whole_sum, shared_sum = whole_term.astype(jnp.float32), shared_term.astype(jnp.float32)
        both_sides(lambda side: gram_copy(1 - side).wait_recv())
        for degree in range(1, TAYLOR + 1):
            whole_term = (apply(whole_term, whole_half) / degree).astype(jnp.bfloat16)
            whole_sum = whole_sum + whole_term.astype(jnp.float32)
            shared_term = (apply(shared_term, shared_half) / degree).astype(jnp.bfloat16)
            shared_sum = shared_sum + shared_term.astype(jnp.float32)
        first = dot(pick[...], whole_sum.astype(jnp.bfloat16), CONTRACT_LAST)
        padded = jnp.concatenate([shared_sum, jnp.zeros((half, orbitals), jnp.float32)], axis=0).astype(jnp.bfloat16)
        second = dot(pick[...], padded, CONTRACT_LAST)
        for index in range(n):
            upper = second[index * height : index * height + height // 2]
            lower = second[index * height + height // 2 : (index + 1) * height]
            outgoing[index, :height] = first[index * height : (index + 1) * height].astype(jnp.bfloat16)
            outgoing[index, height:] = (upper + pltpu.roll(lower, half, 1)).astype(jnp.bfloat16)
        for step in range(1, n):
            peer = lax.rem(me + step, n)
            remote(outgoing.at[peer], incoming.at[mine], out_sems.at[0, step], out_sems.at[1, mine], peer).start()
        incoming[mine] = outgoing[me]

    from_everyone(lambda peer: energy_own, energy_slots, energy_sems)
    energy = energy_slots[0]
    for index in range(1, n):
        energy = energy + energy_slots[index]
    energy_ref[...] = energy
    each_middle(
        lambda number, peer: remote(
            outgoing.at[0], incoming.at[number], out_sems.at[0, 0], out_sems.at[1, number], peer
        ).wait_recv()
    )
    out_lane = lax.broadcasted_iota(jnp.int32, (height, LANES), 1)
    for number in range(0, n // 2, 2):
        halves = []
        for side in range(2):
            got = incoming[number + side].astype(jnp.float32)
            out_ref[number // 2 * 3 + 2 * side] = got[:own_rows].astype(jnp.bfloat16)
            low_part = got[height:]
            moved = pltpu.roll(low_part, half, 1)
            halves.append(jnp.concatenate([moved, low_part] if side else [low_part, moved], axis=0))
        joined = jnp.where(out_lane < half, halves[0], halves[1])
        out_ref[number // 2 * 3 + 1] = joined[:own_rows].astype(jnp.bfloat16)

    for step in (*range(2, n, 2), 1):
        dens_out(step).wait_send()
    for step in range(2, n, 2):
        dens_relay(step).wait_send()
    all_sent(lambda peer: energy_own, energy_slots, energy_sems)
    each_middle(lambda number, peer: field_send(number, peer).wait_send())

    def sent(sems, number, messages, target):
        for message in messages:
            send(me, message, sems.at[number, message], target).wait_send()

    for number in range(2):
        sent(in_sems, number, range(3), inner)
    for number in range(3):
        sent(out_sems_map, number, range(3), outer)
    for number in range(8):
        sent(side_sems, number, range(3), partner)

    @pl.when(is_middle)
    def _():
        both_sides(lambda side: gram_copy(side).wait_send())
        sent(in_sems, 2, (0,), inner)
        sent(across_sems, 0, range(3), across)
        sent(across_sems, 1, range(3), across)
        sent(across_sems, 2, (1, 2), across)
        for step in range(1, n):
            peer = lax.rem(me + step, n)
            remote(
                outgoing.at[peer], incoming.at[mine], out_sems.at[0, step], out_sems.at[1, mine], peer
            ).wait_send()

    @pl.when(is_corner)
    def _():
        sent(out_sems_map, 3, range(3), outer)


def fused(n, points_map, trial, core, walker_major, draws_t):
    rows, orbitals = points_map.shape
    points, occupied = trial.shape
    walker_count = walker_major.shape[0]
    columns = walker_count * occupied
    fold = (rows // (LANES // (orbitals % LANES)) + 15) // 16 * 16
    own, own_rows = columns // (n // 2), orbitals // n
    lines = (walker_count + 1 + 15) // 16 * 16
    span = max((k * own + own - 1) // occupied - k * own // occupied + 1 for k in range(n // 2))
    height = (own_rows + 31) // 32 * 32
    window = (rows + (LANES - 16) + LANES - 1) // LANES * LANES
    full = (points - rows) // LANES * LANES + window
    far = n // 4
    dma = pltpu.SemaphoreType.DMA
    vmem = pltpu.VMEM
    return pl.pallas_call(
        functools.partial(fused_kernel, n, walker_count, own),
        out_shape=(
            jax.ShapeDtypeStruct((walker_count, own_rows, occupied), jnp.bfloat16),
            jax.ShapeDtypeStruct((lines, LANES), jnp.float32),
        ),
        in_specs=[pl.BlockSpec(memory_space=pl.ANY)] * 4 + [pl.BlockSpec(memory_space=pltpu.VMEM)],
        out_specs=[pl.BlockSpec(memory_space=pltpu.VMEM)] * 2,
        scratch_shapes=[
            vmem((points, orbitals), jnp.bfloat16),
            vmem((n, fold, LANES), jnp.bfloat16),
            vmem((points, occupied), jnp.bfloat16),
            vmem((rows, points), jnp.bfloat16),
            vmem((orbitals, columns), jnp.bfloat16),
            vmem((rows, columns), jnp.bfloat16),
            vmem((window, columns), jnp.bfloat16),
            vmem((walker_count, 8, window), jnp.float32),
            vmem((orbitals, 2 * rows), jnp.bfloat16),
            vmem((orbitals, orbitals), jnp.float32),
            vmem((orbitals, orbitals), jnp.float32),
            vmem((orbitals, orbitals), jnp.bfloat16),
            vmem((orbitals, orbitals), jnp.bfloat16),
            vmem((lines, window), jnp.bfloat16),
            vmem((n, lines, window), jnp.bfloat16),
            vmem((lines, full), jnp.float32),
            vmem((lines, window), jnp.float32),
            vmem((n, span, 1, window), jnp.float32),
            vmem((lines, 1, window), jnp.float32),
            vmem((lines, LANES), jnp.float32),
            vmem((n, lines, LANES), jnp.float32),
            vmem((n * height, orbitals), jnp.bfloat16),
            vmem((n, height + height // 2, LANES), jnp.bfloat16),
            vmem((n // 2, height + height // 2, LANES), jnp.bfloat16),
            dma((3 + walker_count,)),
            dma((3, 3)),
            dma((4, 3)),
            dma((3, 3)),
            dma((8, 3)),
            dma((n, 3)),
            dma((2, n)),
            dma((2, n)),
            dma((2, n)),
            dma((2, n)),
            dma((2,)),
        ],
        compiler_params=pltpu.CompilerParams(
            collective_id=0, has_side_effects=True, vmem_limit_bytes=60 * 2**20
        ),
        name="fused",
    )(points_map, trial, core, walker_major, draws_t)


def propagate_kernel(n, occupied, piece, map_ref, field_ref, cols_ref, out_ref, wide, total, term):
    points, orbitals = map_ref.shape
    own = cols_ref.shape[0]
    start = lax.axis_index("pts") * own
    walker_ids = (start + lax.broadcasted_iota(jnp.int32, (1, own), 1)) // occupied
    low = start // occupied
    span = (own + occupied - 2) // occupied + 1
    running = cols_ref[...].astype(jnp.float32)
    term[...] = cols_ref[...]
    for degree in range(1, TAYLOR + 1):
        total[...] = jnp.zeros_like(total)

        @pl.loop(0, points // piece)
        def _(number):
            here = pl.ds(pl.multiple_of(number * piece, piece), piece)
            if degree == 1:
                field = field_ref[here, :]
                lane = lax.broadcasted_iota(jnp.int32, field.shape, 1)
                spread = jnp.zeros((piece, own), jnp.float32)
                for offset in range(span):
                    column = jnp.sum(jnp.where(lane == low + offset, field, 0.0), axis=1, keepdims=True)
                    spread = jnp.where(walker_ids == low + offset, column, spread)
                wide[here, :] = spread
            block = map_ref[here, :]
            current = dot(block, term[...], CONTRACT_LAST).astype(jnp.bfloat16)
            scaled = (wide[here, :] * current.astype(jnp.float32)).astype(jnp.bfloat16)
            total[...] += dot(scaled, block, CONTRACT_FIRST)

        term[...] = (total[...] / degree).astype(jnp.bfloat16)
        running = running + term[...].astype(jnp.float32)
    out_ref[...] = running.astype(jnp.bfloat16)


def propagate(n, occupied, map_full, field_full, own_cols_t):
    points, orbitals = map_full.shape
    own = own_cols_t.shape[0]
    piece = next(p for p in (1280, 640, 256, points // n) if points % p == 0)
    return pl.pallas_call(
        functools.partial(propagate_kernel, n, occupied, piece),
        out_shape=jax.ShapeDtypeStruct((own, orbitals), jnp.bfloat16),
        in_specs=[pl.BlockSpec(memory_space=pltpu.VMEM)] * 3,
        out_specs=pl.BlockSpec(memory_space=pltpu.VMEM),
        scratch_shapes=[
            pltpu.VMEM((points, own), jnp.float32),
            pltpu.VMEM((own, orbitals), jnp.float32),
            pltpu.VMEM((own, orbitals), jnp.bfloat16),
        ],
        cost_estimate=pl.CostEstimate(
            flops=12 * points * orbitals * own, bytes_accessed=2 * map_full.size, transcendentals=0
        ),
        compiler_params=pltpu.CompilerParams(vmem_limit_bytes=60 * 2**20),
        name="propagate",
    )(map_full, field_full, own_cols_t)


def exchange_plain(trial, trial_here, core, orbit):
    core_block = core.astype(jnp.float32)

    def per_walker(operands):
        left_orb, right_orb = operands
        forward = jnp.dot(left_orb, trial.T, preferred_element_type=jnp.float32)
        backward = jnp.dot(trial_here, right_orb.T, preferred_element_type=jnp.float32)
        return jnp.sum(core_block * forward * backward)

    everyone = lax.all_gather(orbit, "pts", axis=0, tiled=True)
    return lax.map(per_walker, (jnp.moveaxis(orbit, 1, 0), jnp.moveaxis(everyone, 1, 0)))


def gather_stacked(part):
    n = lax.axis_size("pts")
    copies = jnp.broadcast_to(part[None], (n,) + part.shape)
    return lax.all_to_all(copies, "pts", split_axis=0, concat_axis=0, tiled=True)


def body(points_map, trial, core, walkers, draws):
    point_rows = points_map.shape[0]
    orbitals = points_map.shape[1]
    walker_count = walkers.shape[1]
    occupied = walkers.shape[2]
    n = lax.axis_size("pts")
    own_rows = orbitals // n
    own_cols = walker_count * occupied // n
    rest = orbitals % LANES
    if point_rows % 16 == 0 and n == 16 and 4 * own_cols == 3 * LANES and orbitals // LANES % 2 == 0 and occupied == LANES and rest and LANES % rest == 0:
        placed, energy = fused(n, points_map, trial, core, jnp.moveaxis(walkers, 1, 0), draws.T)
        return jnp.moveaxis(placed, 0, 1), energy[:walker_count, 0]
    flat_walkers = walkers.reshape(orbitals, walker_count * occupied)
    point_first = lax.axis_index("pts") * point_rows
    trial_here = lax.dynamic_slice_in_dim(trial, point_first, point_rows, 0)
    flat_orbit = jnp.dot(points_map, flat_walkers, preferred_element_type=jnp.float32).astype(jnp.bfloat16)
    orbit = flat_orbit.reshape(point_rows, walker_count, occupied)
    density = (
        jnp.sum(orbit.astype(jnp.float32) * trial_here.astype(jnp.float32)[:, None, :], axis=2)
        / math.sqrt(occupied)
    ).astype(jnp.bfloat16)
    potential = jnp.dot(
        core,
        jnp.moveaxis(gather_stacked(density.T), 2, 1).reshape(point_rows * n, walker_count),
        preferred_element_type=jnp.float32,
    )
    field = FIELD_STEP * (node_lookup(draws) - FIELD_STEP * potential)
    field_full = jnp.moveaxis(gather_stacked(field.T), 2, 1).reshape(point_rows * n, walker_count)
    col_start = lax.axis_index("pts") * own_cols
    cols_walkers = lax.dynamic_slice_in_dim(flat_walkers, col_start, own_cols, 1)
    map_full = lax.all_gather(points_map, "pts", axis=0, tiled=True)
    final_t = propagate(n, occupied, map_full, field_full, cols_walkers.T)
    exchange = exchange_plain(trial, trial_here, core, orbit)
    placed = lax.all_to_all(final_t.T, "pts", split_axis=0, concat_axis=1, tiled=True)
    hartree = jnp.sum(density.astype(jnp.float32) * potential, axis=0)
    total_points = point_rows * n
    energy = jnp.sum(gather_stacked((hartree - exchange / occupied) / (2.0 * total_points)), axis=0)
    return (placed.reshape(own_rows, walker_count, occupied), energy)


def solution(mesh):
    placed = (
        P(("mol", "pts"), None),
        P("mol", None),
        P(("mol", "pts"), None),
        P("mol", None, None),
        P(("mol", "pts"), None),
    )
    return jax.shard_map(
        body,
        mesh=mesh,
        in_specs=placed,
        out_specs=(P(("mol", "pts"), None, None), P("mol")),
        check_vma=False,
    )
```
